8 devices in a mesh: dp: 1 (over z), cz: 2 (over y), cy: 2 (over x), cx: 2 (over core).
Axes of the slice: x: 2, y: 2, z: 1, core: 2. Of those that a mesh axis runs over, the one named last changes fastest.
Arguments:
- x_act: bfloat16 [4096, 2560], P(('dp', 'cx', 'cz'), 'cy')
- w_up: bfloat16 [2560, 10240], P('cy', ('cz', 'cx'))
- w_down: bfloat16 [10240, 2560], P('cz', ('cy', 'cx'))
- z_grad: bfloat16 [4096, 2560], P(('dp', 'cx', 'cz'), 'cy')
Outputs:
- output 1: bfloat16 [4096, 2560], P(('dp', 'cx', 'cz'), 'cy')
- output 2: bfloat16 [2560, 10240], P(('dp', 'cy'), ('cz', 'cx'))
- output 3: bfloat16 [10240, 2560], P(('dp', 'cz'), ('cy', 'cx'))
All inputs are finite; a program needn't handle non-finite values.
Results may differ from the reference program's by a relative error of at most 0.0115215.
Values are sent between devices in bfloat16 or wider.
A program may use at most 1 GiB of HBM per device.

```python
import math
import jax
import jax.numpy as jnp

TOKENS = 4096
MODEL_DIM = 2560
HIDDEN_DIM = 10240
GELU_COEF = 0.044715
SQRT_TWO_PI = math.sqrt(2.0 / math.pi)


def gelu_parts(pre_act):
    inner_arg = SQRT_TWO_PI * (pre_act + GELU_COEF * pre_act * pre_act * pre_act)
    tanh_val = jnp.tanh(inner_arg)
    gelu_val = 0.5 * pre_act * (1.0 + tanh_val)
    gelu_slope = 0.5 * (1.0 + tanh_val) + 0.5 * pre_act * (1.0 - tanh_val * tanh_val) * SQRT_TWO_PI * (1.0 + 3.0 * GELU_COEF * pre_act * pre_act)
    return gelu_val, gelu_slope


def setup_inputs(seed: int = 0, part: int = 0) -> dict:
    base_key = jax.random.key(seed)
    key_up, key_down, key_acts = jax.random.split(base_key, 3)
    part_key = jax.random.fold_in(key_acts, part)
    key_x, key_z = jax.random.split(part_key)
    x_act = jax.random.normal(key_x, (TOKENS, MODEL_DIM), jnp.float32)
    w_up = jax.random.normal(key_up, (MODEL_DIM, HIDDEN_DIM), jnp.float32) * MODEL_DIM ** -0.5
    w_down = jax.random.normal(key_down, (HIDDEN_DIM, MODEL_DIM), jnp.float32) * HIDDEN_DIM ** -0.5
    z_grad = jax.random.normal(key_z, (TOKENS, MODEL_DIM), jnp.float32)
    return {"x_act": x_act.astype(jnp.bfloat16), "w_up": w_up.astype(jnp.bfloat16), "w_down": w_down.astype(jnp.bfloat16), "z_grad": z_grad.astype(jnp.bfloat16)}


def reference(x_act, w_up, w_down, z_grad):
    pre_act = jnp.dot(x_act, w_up, preferred_element_type=jnp.float32).astype(jnp.bfloat16).astype(jnp.float32)
    gelu_val, gelu_slope = gelu_parts(pre_act)
    hidden = gelu_val.astype(jnp.bfloat16)
    h_grad = jnp.dot(z_grad, w_down.T, preferred_element_type=jnp.float32)
    pre_grad = (h_grad * gelu_slope).astype(jnp.bfloat16)
    x_grad = jnp.dot(pre_grad, w_up.T, preferred_element_type=jnp.float32).astype(jnp.bfloat16)
    up_grad = jnp.dot(x_act.T, pre_grad, preferred_element_type=jnp.float32).astype(jnp.bfloat16)
    down_grad = jnp.dot(hidden.T, z_grad, preferred_element_type=jnp.float32).astype(jnp.bfloat16)
    return (x_grad, up_grad, down_grad)
```

```python
import math
import jax
import jax.numpy as jnp
from jax import lax
from jax.experimental import pallas as pl
from jax.experimental.pallas import tpu as pltpu
from jax.sharding import PartitionSpec as P

GELU_COEF = 0.044715
SQRT_TWO_PI = math.sqrt(2.0 / math.pi)
LAST = (((1,), (1,)), ((), ()))
FIRST = (((0,), (0,)), ((), ()))
F32 = jnp.float32
BF16 = jnp.bfloat16
MESH = pl.DeviceIdType.MESH


W = 256
RB = 512
AHEAD = 3
SLOTS = 3


def gelu_parts(c):
    c2 = c * c
    t = jnp.tanh(SQRT_TWO_PI * (c * (1.0 + GELU_COEF * c2)))
    half = 0.5 * (1.0 + t)
    slope = half + 0.5 * c * (1.0 - t * t) * SQRT_TWO_PI * (1.0 + 3.0 * GELU_COEF * c2)
    return c * half, slope


def hidden_kernel(x_in, up, down, z_in,
                  h_out, dc_out, x_out, z_out, dx_own, dx_oth, up_d, up_x, up_xd, down_d, down_x, down_xd,
                  xv, zv, uv, vv, acc, h_st, dc_st,
                  act_send, act_recv, wx_send, wx_recv, wd_send, wd_recv, all_send, all_recv,
                  load_sem, local_sem, out_sem):
    cz, cy, cx = lax.axis_index("cz"), lax.axis_index("cy"), lax.axis_index("cx")
    to_x, to_y, to_d = {"cy": 1 - cy}, {"cz": 1 - cz}, {"cx": 1 - cx}
    rows, dk = x_in.shape
    ffc = up.shape[1]
    dq = down.shape[1]
    chunks = ffc // W

    def remote(src, dst, send, recv, dev):
        return pltpu.make_async_remote_copy(src_ref=src, dst_ref=dst, send_sem=send, recv_sem=recv,
                                            device_id=dev, device_id_type=MESH)

    def mine(c):
        return pl.ds(pl.multiple_of(c * W, W), W)

    def frow(f, c):
        return pl.ds(pl.multiple_of(f * ffc + c * W, W), W)

    own, oth = pl.ds(0, rows), pl.ds(rows, rows)
    near, far = pl.ds(0, dk), pl.ds(dk, dk)

    x1 = remote(x_in, xv.at[own, far], act_send.at[0], act_recv.at[0], to_x)
    z1 = remote(z_in, zv.at[own, far], act_send.at[1], act_recv.at[1], to_x)
    x2 = remote(x_in, xv.at[oth, near], act_send.at[2], act_recv.at[2], to_y)
    z2 = remote(z_in, zv.at[oth, near], act_send.at[3], act_recv.at[3], to_y)
    x3 = remote(xv.at[own, far], xv.at[oth, far], act_send.at[4], act_recv.at[4], to_y)
    z3 = remote(zv.at[own, far], zv.at[oth, far], act_send.at[5], act_recv.at[5], to_y)
    up_all = remote(up, up_d, all_send.at[0], all_recv.at[0], to_d)
    down_all = remote(down, down_d, all_send.at[1], all_recv.at[1], to_d)

    def over_x(c):
        return [remote(up.at[:, mine(c)], up_x.at[:, mine(c)], wx_send.at[c, 0], wx_recv.at[c, 0], to_x)] + [
            remote(down.at[frow(f, c)], down_x.at[frow(f, c)], wx_send.at[c, 1 + f], wx_recv.at[c, 1 + f], to_x)
            for f in range(2)]

    def over_d(c):
        return [remote(up_x.at[:, mine(c)], up_xd.at[:, mine(c)], wd_send.at[c, 0], wd_recv.at[c, 0], to_d)] + [
            remote(down_x.at[frow(f, c)], down_xd.at[frow(f, c)], wd_send.at[c, 1 + f], wd_recv.at[c, 1 + f], to_d)
            for f in range(2)]

    def lanes(part, core):
        return pl.ds(pl.multiple_of(part * dk + core * dq, 128), dq)

    def loads(c, late):
        slot = lax.rem(c, SLOTS)
        left, right = pl.ds(0, W), pl.ds(W, W)
        if late:
            moves = [(up_xd.at[:, mine(c)], uv.at[slot, far, right])]
            parts = [(down_xd, lanes(1, 1 - cx))]
        else:
            moves = [(up.at[:, mine(c)], uv.at[slot, near, left]),
                     (up_d.at[:, mine(c)], uv.at[slot, near, right]),
                     (up_x.at[:, mine(c)], uv.at[slot, far, left])]
            parts = [(down, lanes(0, cx)), (down_d, lanes(0, 1 - cx)), (down_x, lanes(1, cx))]
        for src, lane in parts:
            moves.append((src.at[frow(cx, c)], vv.at[slot, left, lane]))
            moves.append((src.at[frow(1 - cx, c)], vv.at[slot, right, lane]))
        base = 9 if late else 0
        return [pltpu.make_async_copy(s, d, load_sem.at[base + i]) for i, (s, d) in enumerate(moves)]

    barrier = pltpu.get_barrier_semaphore()
    for dev in (to_x, to_y, to_d):
        pl.semaphore_signal(barrier, inc=1, device_id=dev, device_id_type=MESH)
    pl.semaphore_wait(barrier, 3)

    x1.start()
    x2.start()
    z1.start()
    z2.start()
    for c in range(AHEAD):
        for copy in over_x(c):
            copy.start()
    up_all.start()
    down_all.start()
    x0 = pltpu.make_async_copy(x_in, xv.at[own, near], local_sem.at[0])
    z0 = pltpu.make_async_copy(z_in, zv.at[own, near], local_sem.at[1])
    x0.start()
    z0.start()

    @pl.loop(0, 2 * rows // 256)
    def _(i):
        acc[pl.ds(pl.multiple_of(i * 256, 256), 256), :] = jnp.zeros((256, dk), F32)

    x1.wait_recv()
    x3.start()
    z1.wait_recv()
    z3.start()
    x0.wait()
    z0.wait()
    up_all.wait_recv()
    down_all.wait_recv()
    x_save = pltpu.make_async_copy(xv.at[:, near], x_out, local_sem.at[0])
    z_save = pltpu.make_async_copy(zv.at[:, near], z_out, local_sem.at[1])

    def outs(n, c, r0):
        sl = lax.rem(n, 2)
        r = pl.ds(r0, RB)
        moves = []
        for k, (st, dst) in enumerate(((h_st, h_out), (dc_st, dc_out))):
            moves.append(pltpu.make_async_copy(st.at[sl, :, pl.ds(0, W)], dst.at[r, frow(cx, c)], out_sem.at[sl, 2 * k]))
            moves.append(pltpu.make_async_copy(st.at[sl, :, pl.ds(W, W)], dst.at[r, frow(1 - cx, c)], out_sem.at[sl, 2 * k + 1]))
        return moves

    nb = rows // RB
    steps = 2 * chunks

    @pl.loop(0, steps)
    def _(s):
        late = s >= 6
        c = jnp.where(late, 3 + (s - 6) // 2, lax.rem(s, 3))
        half = jnp.where(late, lax.rem(s, 2), s // 3)
        odd = lax.rem(s, 2) == 1
        hc = jnp.where(s < 3, s, 3 + (s - 5) // 2)

        @pl.when((s < 3) | ((s >= 5) & odd & (s < steps - 1)))
        def _():
            for copy in over_x(hc):
                copy.wait_recv()
            for copy in over_d(hc):
                copy.start()

            @pl.when(hc + AHEAD < chunks)
            def _():
                for copy in over_x(hc + AHEAD):
                    copy.start()

            for copy in loads(hc, False):
                copy.start()

        @pl.when((s < 3) | (late & ~odd))
        def _():
            for copy in over_d(c):
                copy.wait_recv()
            for copy in loads(c, True):
                copy.start()
            for copy in loads(c, False) + loads(c, True):
                copy.wait()

        @pl.when(s == 3)
        def _():
            x2.wait_recv()
            z2.wait_recv()
            x_save.start()
            z_save.start()
            x3.wait_recv()
            z3.wait_recv()

        slot = lax.rem(c, SLOTS)

        @pl.loop(0, nb)
        def _(b):
            r0 = pl.multiple_of(half * rows + b * RB, RB)
            n = s * nb + b
            sl = lax.rem(n, 2)
            cc = jnp.dot(xv[pl.ds(r0, RB), :], uv[slot], preferred_element_type=F32)
            dh = lax.dot_general(zv[pl.ds(r0, RB), :], vv[slot], LAST, preferred_element_type=F32)
            h, slope = gelu_parts(cc.astype(BF16).astype(F32))
            dc = (dh * slope).astype(BF16)

            @pl.when(n >= 2)
            def _():
                for copy in outs(n, c, r0):
                    copy.wait()

            h_st[sl] = h.astype(BF16)
            dc_st[sl] = dc
            for copy in outs(n, c, r0):
                copy.start()
            acc[pl.ds(r0, RB), :] += lax.dot_general(dc, uv[slot, near, :], LAST, preferred_element_type=F32)

    save = [pltpu.make_async_copy(acc.at[own], dx_own, load_sem.at[0]),
            pltpu.make_async_copy(acc.at[oth], dx_oth, load_sem.at[1])]
    for copy in save:
        copy.start()
    for n in range(2):
        for copy in outs(n, 0, 0):
            copy.wait()
    x_save.wait()
    z_save.wait()
    for copy in (x1, z1, x2, z2, x3, z3, up_all, down_all):
        copy.wait_send()

    @pl.loop(0, chunks)
    def _(c):
        for copy in over_x(c) + over_d(c):
            copy.wait_send()

    for copy in save:
        copy.wait()


def hidden_call(x_act, w_up, w_down, z_grad):
    rows, dk = x_act.shape
    ffc = w_up.shape[1]
    ff, _ = w_down.shape
    chunks = ffc // W
    flops = 2 * rows * 2 * ff * dk * 5
    hbm = pl.BlockSpec(memory_space=pl.ANY)
    sds = jax.ShapeDtypeStruct
    out_shape = [
        sds((2 * rows, ff), BF16), sds((2 * rows, ff), BF16),
        sds((2 * rows, dk), BF16), sds((2 * rows, dk), BF16),
        sds((rows, dk), F32), sds((rows, dk), F32),
        sds(w_up.shape, BF16), sds(w_up.shape, BF16), sds(w_up.shape, BF16),
        sds(w_down.shape, BF16), sds(w_down.shape, BF16), sds(w_down.shape, BF16),
    ]
    dma = pltpu.SemaphoreType.DMA
    return pl.pallas_call(
        hidden_kernel,
        in_specs=[hbm] * 4,
        out_specs=[hbm] * len(out_shape),
        out_shape=out_shape,
        scratch_shapes=[
            pltpu.VMEM((2 * rows, 2 * dk), BF16), pltpu.VMEM((2 * rows, 2 * dk), BF16),
            pltpu.VMEM((SLOTS, 2 * dk, 2 * W), BF16), pltpu.VMEM((SLOTS, 2 * W, 2 * dk), BF16),
            pltpu.VMEM((2 * rows, dk), F32),
            pltpu.VMEM((2, RB, 2 * W), BF16), pltpu.VMEM((2, RB, 2 * W), BF16),
            dma((6,)), dma((6,)), dma((chunks, 3)), dma((chunks, 3)), dma((chunks, 3)), dma((chunks, 3)),
            dma((2,)), dma((2,)), dma((12,)), dma((2,)), dma((2, 4)),
        ],
        compiler_params=pltpu.CompilerParams(
            collective_id=0, has_side_effects=True, vmem_limit_bytes=67_000_000),
        cost_estimate=pl.CostEstimate(flops=flops, bytes_accessed=200_000_000, transcendentals=2 * rows * ff),
        name="hidden",
    )(x_act, w_up, w_down, z_grad)


def solution(mesh):
    row_spec = P(("dp", "cx", "cz"), "cy")
    up_spec = P("cy", ("cz", "cx"))
    down_spec = P("cz", ("cy", "cx"))
    up_out = P(("dp", "cy"), ("cz", "cx"))
    down_out = P(("dp", "cz"), ("cy", "cx"))
    swap = [(0, 1), (1, 0)]

    def local_step(x_act, w_up, w_down, z_grad):
        h, dc, xs, zs, dx_own, dx_oth = hidden_call(x_act, w_up, w_down, z_grad)[:6]
        got = lax.ppermute(dx_oth, "cz", swap)
        down_part = lax.dot_general(h, zs, FIRST, preferred_element_type=F32)
        up_part = lax.dot_general(xs, dc, FIRST, preferred_element_type=F32)
        down_sum = lax.psum_scatter(down_part, "cx", scatter_dimension=1, tiled=True)
        up_sum = lax.psum_scatter(up_part, "cx", scatter_dimension=1, tiled=True)
        down_grad = down_sum.astype(BF16)
        up_grad = up_sum.astype(BF16)
        x_grad = (dx_own + got).astype(BF16)
        return (x_grad, up_grad, down_grad)

    return jax.shard_map(local_step, mesh=mesh, in_specs=(row_spec, up_spec, down_spec, row_spec), out_specs=(row_spec, up_out, down_out), check_vma=False)
```

```python
import math
import jax
import jax.numpy as jnp
from jax import lax
from jax.experimental import pallas as pl
from jax.experimental.pallas import tpu as pltpu
from jax.sharding import PartitionSpec as P

GELU_COEF = 0.044715
SQRT_TWO_PI = math.sqrt(2.0 / math.pi)
LAST = (((1,), (1,)), ((), ()))
FIRST = (((0,), (0,)), ((), ()))
F32 = jnp.float32
BF16 = jnp.bfloat16
MESH = pl.DeviceIdType.MESH


W = 128
RB = 1024
AHEAD = 6
SLOTS = 6


def gelu_parts(c):
    c2 = c * c
    t = jnp.tanh(SQRT_TWO_PI * (c * (1.0 + GELU_COEF * c2)))
    half = 0.5 * (1.0 + t)
    slope = half + 0.5 * c * (1.0 - t * t) * SQRT_TWO_PI * (1.0 + 3.0 * GELU_COEF * c2)
    return c * half, slope


def hidden_kernel(x_in, up, down, z_in,
                  h_out, dc_own, dc_oth, x_out, z_own, z_oth, dx_own, dx_oth, up_d, up_x, up_xd, down_d, down_x, down_xd,
                  xv, zv, uv, vv, acc, h_st, dc_st,
                  act_send, act_recv, wx_send, wx_recv, wd_send, wd_recv, all_send, all_recv,
                  load_sem, local_sem, out_sem):
    cz, cy, cx = lax.axis_index("cz"), lax.axis_index("cy"), lax.axis_index("cx")
    to_x, to_y, to_d = {"cy": 1 - cy}, {"cz": 1 - cz}, {"cx": 1 - cx}
    rows, dk = x_in.shape
    ffc = up.shape[1]
    dq = down.shape[1]
    chunks = ffc // W

    def remote(src, dst, send, recv, dev):
        return pltpu.make_async_remote_copy(src_ref=src, dst_ref=dst, send_sem=send, recv_sem=recv,
                                            device_id=dev, device_id_type=MESH)

    def mine(c):
        return pl.ds(pl.multiple_of(c * W, W), W)

    def frow(f, c):
        return pl.ds(pl.multiple_of(f * ffc + c * W, W), W)

    own, oth = pl.ds(0, rows), pl.ds(rows, rows)
    near, far = pl.ds(0, dk), pl.ds(dk, dk)

    x1 = remote(x_in, xv.at[own, far], act_send.at[0], act_recv.at[0], to_x)
    z1 = remote(z_in, zv.at[own, far], act_send.at[1], act_recv.at[1], to_x)
    x2 = remote(x_in, xv.at[oth, near], act_send.at[2], act_recv.at[2], to_y)
    z2 = remote(z_in, zv.at[oth, near], act_send.at[3], act_recv.at[3], to_y)
    x3 = remote(xv.at[own, far], xv.at[oth, far], act_send.at[4], act_recv.at[4], to_y)
    z3 = remote(zv.at[own, far], zv.at[oth, far], act_send.at[5], act_recv.at[5], to_y)
    up_all = remote(up, up_d, all_send.at[0], all_recv.at[0], to_d)
    down_all = remote(down, down_d, all_send.at[1], all_recv.at[1], to_d)

    def over_x(c):
        return [remote(up.at[:, mine(c)], up_x.at[:, mine(c)], wx_send.at[c, 0], wx_recv.at[c, 0], to_x)] + [
            remote(down.at[frow(f, c)], down_x.at[frow(f, c)], wx_send.at[c, 1 + f], wx_recv.at[c, 1 + f], to_x)
            for f in range(2)]

    def over_d(c):
        return [remote(up_x.at[:, mine(c)], up_xd.at[:, mine(c)], wd_send.at[c, 0], wd_recv.at[c, 0], to_d)] + [
            remote(down_x.at[frow(f, c)], down_xd.at[frow(f, c)], wd_send.at[c, 1 + f], wd_recv.at[c, 1 + f], to_d)
            for f in range(2)]

    def lanes(part, core):
        return pl.ds(pl.multiple_of(part * dk + core * dq, 128), dq)

    def loads(c, late):
        slot = lax.rem(c, SLOTS)
        left, right = pl.ds(0, W), pl.ds(W, W)
        if late:
            moves = [(up_xd.at[:, mine(c)], uv.at[slot, far, right])]
            parts = [(down_xd, lanes(1, 1 - cx))]
        else:
            moves = [(up.at[:, mine(c)], uv.at[slot, near, left]),
                     (up_d.at[:, mine(c)], uv.at[slot, near, right]),
                     (up_x.at[:, mine(c)], uv.at[slot, far, left])]
            parts = [(down, lanes(0, cx)), (down_d, lanes(0, 1 - cx)), (down_x, lanes(1, cx))]
        for src, lane in parts:
            moves.append((src.at[frow(cx, c)], vv.at[slot, left, lane]))
            moves.append((src.at[frow(1 - cx, c)], vv.at[slot, right, lane]))
        base = 9 if late else 0
        return [pltpu.make_async_copy(s, d, load_sem.at[base + i]) for i, (s, d) in enumerate(moves)]

    barrier = pltpu.get_barrier_semaphore()
    for dev in (to_x, to_y, to_d):
        pl.semaphore_signal(barrier, inc=1, device_id=dev, device_id_type=MESH)
    pl.semaphore_wait(barrier, 3)

    x1.start()
    x2.start()
    z1.start()
    z2.start()
    for c in range(AHEAD):
        for copy in over_x(c):
            copy.start()
    up_all.start()
    down_all.start()
    x0 = pltpu.make_async_copy(x_in, xv.at[own, near], local_sem.at[0])
    z0 = pltpu.make_async_copy(z_in, zv.at[own, near], local_sem.at[1])
    x0.start()
    z0.start()

    @pl.loop(0, 2 * rows // 256)
    def _(i):
        acc[pl.ds(pl.multiple_of(i * 256, 256), 256), :] = jnp.zeros((256, dk), F32)

    x1.wait_recv()
    x3.start()
    z1.wait_recv()
    z3.start()
    x0.wait()
    z0.wait()
    up_all.wait_recv()
    down_all.wait_recv()
    x_save = pltpu.make_async_copy(xv.at[:, near], x_out, local_sem.at[0])
    z_save = [pltpu.make_async_copy(zv.at[:, lanes(0, cx)], z_own, local_sem.at[1]),
              pltpu.make_async_copy(zv.at[:, lanes(0, 1 - cx)], z_oth, local_sem.at[2])]

    def outs(n, c, r0):
        sl = lax.rem(n, 2)
        r = pl.ds(r0, RB)
        left, right = pl.ds(0, W), pl.ds(W, W)
        moves = ((h_st.at[sl, :, left], h_out.at[r, frow(cx, c)]), (h_st.at[sl, :, right], h_out.at[r, frow(1 - cx, c)]),
                 (dc_st.at[sl, :, left], dc_own.at[r, mine(c)]), (dc_st.at[sl, :, right], dc_oth.at[r, mine(c)]))
        return [pltpu.make_async_copy(src, dst, out_sem.at[sl, i]) for i, (src, dst) in enumerate(moves)]

    nb = rows // RB
    steps = 2 * chunks

    @pl.loop(0, steps)
    def _(s):
        late = s >= 2 * SLOTS
        c = jnp.where(late, SLOTS + (s - 2 * SLOTS) // 2, lax.rem(s, SLOTS))
        half = jnp.where(late, lax.rem(s, 2), s // SLOTS)
        odd = lax.rem(s, 2) == 1
        hc = jnp.where(s < SLOTS, s, SLOTS + (s - 2 * SLOTS + 1) // 2)

        @pl.when((s < SLOTS) | ((s >= 2 * SLOTS - 1) & odd & (s < steps - 1)))
        def _():
            for copy in over_x(hc):
                copy.wait_recv()
            for copy in over_d(hc):
                copy.start()

            @pl.when(hc + AHEAD < chunks)
            def _():
                for copy in over_x(hc + AHEAD):
                    copy.start()

            for copy in loads(hc, False):
                copy.start()

        @pl.when((s < SLOTS) | (late & ~odd))
        def _():
            for copy in over_d(c):
                copy.wait_recv()
            for copy in loads(c, True):
                copy.start()
            for copy in loads(c, False) + loads(c, True):
                copy.wait()

        @pl.when(s == SLOTS)
        def _():
            x2.wait_recv()
            z2.wait_recv()
            x_save.start()
            for copy in z_save:
                copy.start()
            x3.wait_recv()
            z3.wait_recv()

        slot = lax.rem(c, SLOTS)

        @pl.loop(0, nb)
        def _(b):
            r0 = pl.multiple_of(half * rows + b * RB, RB)
            n = s * nb + b
            sl = lax.rem(n, 2)
            cc = jnp.dot(xv[pl.ds(r0, RB), :], uv[slot], preferred_element_type=F32)
            dh = lax.dot_general(zv[pl.ds(r0, RB), :], vv[slot], LAST, preferred_element_type=F32)
            h, slope = gelu_parts(cc.astype(BF16).astype(F32))
            dc = (dh * slope).astype(BF16)

            @pl.when(n >= 2)
            def _():
                for copy in outs(n, c, r0):
                    copy.wait()

            h_st[sl] = h.astype(BF16)
            dc_st[sl] = dc
            for copy in outs(n, c, r0):
                copy.start()
            acc[pl.ds(r0, RB), :] += lax.dot_general(dc, uv[slot, near, :], LAST, preferred_element_type=F32)

    save = [pltpu.make_async_copy(acc.at[own], dx_own, load_sem.at[0]),
            pltpu.make_async_copy(acc.at[oth], dx_oth, load_sem.at[1])]
    for copy in save:
        copy.start()
    for n in range(2):
        for copy in outs(n, 0, 0):
            copy.wait()
    x_save.wait()
    for copy in z_save:
        copy.wait()
    for copy in (x1, z1, x2, z2, x3, z3, up_all, down_all):
        copy.wait_send()

    @pl.loop(0, chunks)
    def _(c):
        for copy in over_x(c) + over_d(c):
            copy.wait_send()

    for copy in save:
        copy.wait()


def hidden_call(x_act, w_up, w_down, z_grad):
    rows, dk = x_act.shape
    ffc = w_up.shape[1]
    ff, dq = w_down.shape
    chunks = ffc // W
    flops = 2 * rows * 2 * ff * dk * 5
    hbm = pl.BlockSpec(memory_space=pl.ANY)
    sds = jax.ShapeDtypeStruct
    out_shape = [
        sds((2 * rows, ff), BF16), sds((2 * rows, ffc), BF16), sds((2 * rows, ffc), BF16),
        sds((2 * rows, dk), BF16), sds((2 * rows, dq), BF16), sds((2 * rows, dq), BF16),
        sds((rows, dk), F32), sds((rows, dk), F32),
        sds(w_up.shape, BF16), sds(w_up.shape, BF16), sds(w_up.shape, BF16),
        sds(w_down.shape, BF16), sds(w_down.shape, BF16), sds(w_down.shape, BF16),
    ]
    dma = pltpu.SemaphoreType.DMA
    return pl.pallas_call(
        hidden_kernel,
        in_specs=[hbm] * 4,
        out_specs=[hbm] * len(out_shape),
        out_shape=out_shape,
        scratch_shapes=[
            pltpu.VMEM((2 * rows, 2 * dk), BF16), pltpu.VMEM((2 * rows, 2 * dk), BF16),
            pltpu.VMEM((SLOTS, 2 * dk, 2 * W), BF16), pltpu.VMEM((SLOTS, 2 * W, 2 * dk), BF16),
            pltpu.VMEM((2 * rows, dk), F32),
            pltpu.VMEM((2, RB, 2 * W), BF16), pltpu.VMEM((2, RB, 2 * W), BF16),
            dma((6,)), dma((6,)), dma((chunks, 3)), dma((chunks, 3)), dma((chunks, 3)), dma((chunks, 3)),
            dma((2,)), dma((2,)), dma((12,)), dma((3,)), dma((2, 4)),
        ],
        compiler_params=pltpu.CompilerParams(
            collective_id=0, has_side_effects=True, vmem_limit_bytes=67_000_000),
        cost_estimate=pl.CostEstimate(flops=flops, bytes_accessed=200_000_000, transcendentals=2 * rows * ff),
        name="hidden",
    )(x_act, w_up, w_down, z_grad)


def solution(mesh):
    row_spec = P(("dp", "cx", "cz"), "cy")
    up_spec = P("cy", ("cz", "cx"))
    down_spec = P("cz", ("cy", "cx"))
    up_out = P(("dp", "cy"), ("cz", "cx"))
    down_out = P(("dp", "cz"), ("cy", "cx"))
    swap = [(0, 1), (1, 0)]

    def local_step(x_act, w_up, w_down, z_grad):
        h, dc_own, dc_oth, xs, z_own, z_oth, dx_own, dx_oth = hidden_call(x_act, w_up, w_down, z_grad)[:8]
        got = lax.ppermute(dx_oth, "cz", swap)
        down_part = lax.dot_general(h, z_oth, FIRST, preferred_element_type=F32)
        up_part = lax.dot_general(xs, dc_oth, FIRST, preferred_element_type=F32)
        down_got = lax.ppermute(down_part, "cx", swap)
        up_got = lax.ppermute(up_part, "cx", swap)
        down_grad = (lax.dot_general(h, z_own, FIRST, preferred_element_type=F32) + down_got).astype(BF16)
        up_grad = (lax.dot_general(xs, dc_own, FIRST, preferred_element_type=F32) + up_got).astype(BF16)
        x_grad = (dx_own + got).astype(BF16)
        return (x_grad, up_grad, down_grad)

    return jax.shard_map(local_step, mesh=mesh, in_specs=(row_spec, up_spec, down_spec, row_spec), out_specs=(row_spec, up_out, down_out), check_vma=False)
```

```python
import math
import jax
import jax.numpy as jnp
from jax import lax
from jax.experimental import pallas as pl
from jax.experimental.pallas import tpu as pltpu
from jax.sharding import PartitionSpec as P

GELU_COEF = 0.044715
SQRT_TWO_PI = math.sqrt(2.0 / math.pi)
LAST = (((1,), (1,)), ((), ()))
FIRST = (((0,), (0,)), ((), ()))
F32 = jnp.float32
BF16 = jnp.bfloat16
MESH = pl.DeviceIdType.MESH


W = 128
RB = 1024
PHI = 8
AHEAD = 6
SLOTS = 6


def gelu_parts(c):
    c2 = c * c
    t = jnp.tanh(SQRT_TWO_PI * (c * (1.0 + GELU_COEF * c2)))
    half = 0.5 * (1.0 + t)
    slope = half + 0.5 * c * (1.0 - t * t) * SQRT_TWO_PI * (1.0 + 3.0 * GELU_COEF * c2)
    return c * half, slope


def hidden_kernel(x_in, up, down, z_in,
                  h_out, dc_own, dc_oth, x_out, z_own, z_oth, dx_own, dx_part, dx_got, dcp_own, dcp_oth, up_y, up_yd, up_d, up_x, up_xd, down_d, down_x, down_xd,
                  xv, zv, uv, vv, acc, h_st, dc_st,
                  act_send, act_recv, wx_send, wx_recv, wd_send, wd_recv, all_send, all_recv,
                  load_sem, local_sem, out_sem, extra_sem):
    cz, cy, cx = lax.axis_index("cz"), lax.axis_index("cy"), lax.axis_index("cx")
    to_x, to_y, to_d = {"cy": 1 - cy}, {"cz": 1 - cz}, {"cx": 1 - cx}
    rows, dk = x_in.shape
    ffc = up.shape[1]
    dq = down.shape[1]
    chunks = ffc // W

    def remote(src, dst, send, recv, dev):
        return pltpu.make_async_remote_copy(src_ref=src, dst_ref=dst, send_sem=send, recv_sem=recv,
                                            device_id=dev, device_id_type=MESH)

    def mine(c):
        return pl.ds(pl.multiple_of(c * W, W), W)

    def frow(f, c):
        return pl.ds(pl.multiple_of(f * ffc + c * W, W), W)

    own, oth = pl.ds(0, rows), pl.ds(rows, rows)
    near, far = pl.ds(0, dk), pl.ds(dk, dk)

    x1 = remote(x_in, xv.at[own, far], act_send.at[0], act_recv.at[0], to_x)
    z1 = remote(z_in, zv.at[own, far], act_send.at[1], act_recv.at[1], to_x)
    x2 = remote(x_in, xv.at[oth, near], act_send.at[2], act_recv.at[2], to_y)
    z2 = remote(z_in, zv.at[oth, near], act_send.at[3], act_recv.at[3], to_y)
    x3 = remote(xv.at[own, far], xv.at[oth, far], act_send.at[4], act_recv.at[4], to_y)
    z3 = remote(zv.at[own, far], zv.at[oth, far], act_send.at[5], act_recv.at[5], to_y)
    up_all = remote(up, up_d, all_send.at[0], all_recv.at[0], to_d)
    down_all = remote(down, down_d, all_send.at[1], all_recv.at[1], to_d)

    split = chunks - PHI
    tail = pl.ds(split * W, PHI * W)
    up_tail = remote(up.at[:, tail], up_y, all_send.at[2], all_recv.at[2], to_y)
    up_tail_d = remote(up_y, up_yd, all_send.at[3], all_recv.at[3], to_d)
    part_save = pltpu.make_async_copy(acc.at[oth], dx_part, local_sem.at[3])
    part_send = remote(dx_part, dx_got, all_send.at[4], all_recv.at[4], to_y)
    own_save = pltpu.make_async_copy(acc.at[own], dx_own, local_sem.at[4])

    def over_x(c):
        return [remote(up.at[:, mine(c)], up_x.at[:, mine(c)], wx_send.at[c, 0], wx_recv.at[c, 0], to_x)] + [
            remote(down.at[frow(f, c)], down_x.at[frow(f, c)], wx_send.at[c, 1 + f], wx_recv.at[c, 1 + f], to_x)
            for f in range(2)]

    def over_d(c):
        return [remote(up_x.at[:, mine(c)], up_xd.at[:, mine(c)], wd_send.at[c, 0], wd_recv.at[c, 0], to_d)] + [
            remote(down_x.at[frow(f, c)], down_xd.at[frow(f, c)], wd_send.at[c, 1 + f], wd_recv.at[c, 1 + f], to_d)
            for f in range(2)]

    def lanes(part, core):
        return pl.ds(pl.multiple_of(part * dk + core * dq, 128), dq)

    def loads(c, late):
        slot = lax.rem(c, SLOTS)
        left, right = pl.ds(0, W), pl.ds(W, W)
        if late:
            moves = [(up_xd.at[:, mine(c)], uv.at[slot, far, right])]
            parts = [(down_xd, lanes(1, 1 - cx))]
        else:
            moves = [(up.at[:, mine(c)], uv.at[slot, near, left]),
                     (up_d.at[:, mine(c)], uv.at[slot, near, right]),
                     (up_x.at[:, mine(c)], uv.at[slot, far, left])]
            parts = [(down, lanes(0, cx)), (down_d, lanes(0, 1 - cx)), (down_x, lanes(1, cx))]
        for src, lane in parts:
            moves.append((src.at[frow(cx, c)], vv.at[slot, left, lane]))
            moves.append((src.at[frow(1 - cx, c)], vv.at[slot, right, lane]))
        base = 9 if late else 0
        return [pltpu.make_async_copy(s, d, load_sem.at[base + i]) for i, (s, d) in enumerate(moves)]

    barrier = pltpu.get_barrier_semaphore()
    for dev in (to_x, to_y, to_d):
        pl.semaphore_signal(barrier, inc=1, device_id=dev, device_id_type=MESH)
    pl.semaphore_wait(barrier, 3)

    x1.start()
    x2.start()
    z1.start()
    z2.start()
    for c in range(AHEAD):
        for copy in over_x(c):
            copy.start()
    up_all.start()
    down_all.start()
    x0 = pltpu.make_async_copy(x_in, xv.at[own, near], local_sem.at[0])
    z0 = pltpu.make_async_copy(z_in, zv.at[own, near], local_sem.at[1])
    x0.start()
    z0.start()

    @pl.loop(0, 2 * rows // 256)
    def _(i):
        acc[pl.ds(pl.multiple_of(i * 256, 256), 256), :] = jnp.zeros((256, dk), F32)

    x1.wait_recv()
    x3.start()
    z1.wait_recv()
    z3.start()
    up_tail.start()
    x0.wait()
    z0.wait()
    up_all.wait_recv()
    down_all.wait_recv()
    x_save = pltpu.make_async_copy(xv.at[:, near], x_out, local_sem.at[0])
    z_save = [pltpu.make_async_copy(zv.at[:, lanes(0, cx)], z_own, local_sem.at[1]),
              pltpu.make_async_copy(zv.at[:, lanes(0, 1 - cx)], z_oth, local_sem.at[2])]

    def outs(n, c, r0):
        sl = lax.rem(n, 2)
        r = pl.ds(r0, RB)
        left, right = pl.ds(0, W), pl.ds(W, W)
        moves = ((h_st.at[sl, :, left], h_out.at[r, frow(cx, c)]), (h_st.at[sl, :, right], h_out.at[r, frow(1 - cx, c)]),
                 (dc_st.at[sl, :, left], dc_own.at[r, mine(c)]), (dc_st.at[sl, :, right], dc_oth.at[r, mine(c)]))
        return [pltpu.make_async_copy(src, dst, out_sem.at[sl, i]) for i, (src, dst) in enumerate(moves)]

    def extra(n, c):
        sl = lax.rem(n, 2)
        cols = pl.ds(pl.multiple_of((c - split) * W, W), W)
        return [pltpu.make_async_copy(dc_st.at[sl, :, pl.ds(0, W)], dcp_own.at[:, cols], extra_sem.at[0]),
                pltpu.make_async_copy(dc_st.at[sl, :, pl.ds(W, W)], dcp_oth.at[:, cols], extra_sem.at[1])]

    steps = 2 * chunks

    @pl.loop(0, steps)
    def _(s):
        late = s >= 2 * SLOTS
        c = jnp.where(late, SLOTS + (s - 2 * SLOTS) // 2, lax.rem(s, SLOTS))
        half = jnp.where(late, lax.rem(s, 2), s // SLOTS)
        odd = lax.rem(s, 2) == 1
        hc = jnp.where(s < SLOTS, s, SLOTS + (s - 2 * SLOTS + 1) // 2)

        @pl.when((s < SLOTS) | ((s >= 2 * SLOTS - 1) & odd & (s < steps - 1)))
        def _():
            for copy in over_x(hc):
                copy.wait_recv()
            for copy in over_d(hc):
                copy.start()

            @pl.when(hc + AHEAD < chunks)
            def _():
                for copy in over_x(hc + AHEAD):
                    copy.start()

            for copy in loads(hc, False):
                copy.start()

        @pl.when((s < SLOTS) | (late & ~odd))
        def _():
            for copy in over_d(c):
                copy.wait_recv()
            for copy in loads(c, True):
                copy.start()
            for copy in loads(c, False) + loads(c, True):
                copy.wait()

        @pl.when(s == SLOTS)
        def _():
            x2.wait_recv()
            z2.wait_recv()
            x_save.start()
            for copy in z_save:
                copy.start()
            x3.wait_recv()
            z3.wait_recv()

        @pl.when(s == 2 * split)
        def _():
            part_save.start()
            up_tail.wait_recv()
            up_tail_d.start()
            part_save.wait()
            part_send.start()

        @pl.when(s == steps - 1)
        def _():
            own_save.start()

        slot = lax.rem(c, SLOTS)
        r0 = pl.multiple_of(half * rows, RB)
        sl = lax.rem(s, 2)
        cc = jnp.dot(xv[pl.ds(r0, RB), :], uv[slot], preferred_element_type=F32)
        dh = lax.dot_general(zv[pl.ds(r0, RB), :], vv[slot], LAST, preferred_element_type=F32)
        h, slope = gelu_parts(cc.astype(BF16).astype(F32))
        dc = (dh * slope).astype(BF16)

        @pl.when(s >= 2)
        def _():
            for copy in outs(s, c, r0):
                copy.wait()

        @pl.when((s >= 2 * split + 3) & odd)
        def _():
            for copy in extra(s, c):
                copy.wait()

        h_st[sl] = h.astype(BF16)
        dc_st[sl] = dc
        for copy in outs(s, c, r0):
            copy.start()

        @pl.when((half == 0) | (c < split))
        def _():
            acc[pl.ds(r0, RB), :] += lax.dot_general(dc_st[sl], uv[slot, near, :], LAST, preferred_element_type=F32)

        @pl.when((half == 1) & (c >= split))
        def _():
            for copy in extra(s, c):
                copy.start()

    for n in range(2):
        for copy in outs(n, 0, 0):
            copy.wait()
    for copy in extra(1, split):
        copy.wait()
    own_save.wait()
    up_tail_d.wait_recv()
    part_send.wait_recv()
    x_save.wait()
    for copy in z_save:
        copy.wait()
    for copy in (x1, z1, x2, z2, x3, z3, up_all, down_all, up_tail, up_tail_d, part_send):
        copy.wait_send()

    @pl.loop(0, chunks)
    def _(c):
        for copy in over_x(c) + over_d(c):
            copy.wait_send()


def hidden_call(x_act, w_up, w_down, z_grad):
    rows, dk = x_act.shape
    ffc = w_up.shape[1]
    ff, dq = w_down.shape
    chunks = ffc // W
    flops = 2 * rows * 2 * ff * dk * 5
    hbm = pl.BlockSpec(memory_space=pl.ANY)
    sds = jax.ShapeDtypeStruct
    out_shape = [
        sds((2 * rows, ff), BF16), sds((2 * rows, ffc), BF16), sds((2 * rows, ffc), BF16),
        sds((2 * rows, dk), BF16), sds((2 * rows, dq), BF16), sds((2 * rows, dq), BF16),
        sds((rows, dk), F32), sds((rows, dk), F32), sds((rows, dk), F32),
        sds((rows, PHI * W), BF16), sds((rows, PHI * W), BF16), sds((dk, PHI * W), BF16), sds((dk, PHI * W), BF16),
        sds(w_up.shape, BF16), sds(w_up.shape, BF16), sds(w_up.shape, BF16),
        sds(w_down.shape, BF16), sds(w_down.shape, BF16), sds(w_down.shape, BF16),
    ]
    dma = pltpu.SemaphoreType.DMA
    return pl.pallas_call(
        hidden_kernel,
        in_specs=[hbm] * 4,
        out_specs=[hbm] * len(out_shape),
        out_shape=out_shape,
        scratch_shapes=[
            pltpu.VMEM((2 * rows, 2 * dk), BF16), pltpu.VMEM((2 * rows, 2 * dk), BF16),
            pltpu.VMEM((SLOTS, 2 * dk, 2 * W), BF16), pltpu.VMEM((SLOTS, 2 * W, 2 * dk), BF16),
            pltpu.VMEM((2 * rows, dk), F32),
            pltpu.VMEM((2, RB, 2 * W), BF16), pltpu.VMEM((2, RB, 2 * W), BF16),
            dma((6,)), dma((6,)), dma((chunks, 3)), dma((chunks, 3)), dma((chunks, 3)), dma((chunks, 3)),
            dma((5,)), dma((5,)), dma((12,)), dma((5,)), dma((2, 4)), dma((2,)),
        ],
        compiler_params=pltpu.CompilerParams(
            collective_id=0, has_side_effects=True, vmem_limit_bytes=67_000_000),
        cost_estimate=pl.CostEstimate(flops=flops, bytes_accessed=200_000_000, transcendentals=2 * rows * ff),
        name="hidden",
    )(x_act, w_up, w_down, z_grad)


def solution(mesh):
    row_spec = P(("dp", "cx", "cz"), "cy")
    up_spec = P("cy", ("cz", "cx"))
    down_spec = P("cz", ("cy", "cx"))
    up_out = P(("dp", "cy"), ("cz", "cx"))
    down_out = P(("dp", "cz"), ("cy", "cx"))
    swap = [(0, 1), (1, 0)]

    def local_step(x_act, w_up, w_down, z_grad):
        (h, dc_own, dc_oth, xs, z_own, z_oth, dx_own, _, dx_got, dcp_own, dcp_oth, up_y, up_yd) = hidden_call(
            x_act, w_up, w_down, z_grad)[:13]
        dcr_own = lax.ppermute(dcp_own, "cz", swap)
        dcr_oth = lax.ppermute(dcp_oth, "cz", swap)
        down_part = lax.dot_general(h, z_oth, FIRST, preferred_element_type=F32)
        up_part = lax.dot_general(xs, dc_oth, FIRST, preferred_element_type=F32)
        down_got = lax.ppermute(down_part, "cx", swap)
        up_got = lax.ppermute(up_part, "cx", swap)
        down_grad = (lax.dot_general(h, z_own, FIRST, preferred_element_type=F32) + down_got).astype(BF16)
        up_grad = (lax.dot_general(xs, dc_own, FIRST, preferred_element_type=F32) + up_got).astype(BF16)
        dx = lax.dot_general(dcr_own, up_y, LAST, preferred_element_type=F32) + (dx_own + dx_got)
        x_grad = (lax.dot_general(dcr_oth, up_yd, LAST, preferred_element_type=F32) + dx).astype(BF16)
        return (x_grad, up_grad, down_grad)

    return jax.shard_map(local_step, mesh=mesh, in_specs=(row_spec, up_spec, down_spec, row_spec), out_specs=(row_spec, up_out, down_out), check_vma=False)
```

```python
import math
import jax
import jax.numpy as jnp
from jax import lax
from jax.experimental import pallas as pl
from jax.experimental.pallas import tpu as pltpu
from jax.sharding import PartitionSpec as P

GELU_COEF = 0.044715
SQRT_TWO_PI = math.sqrt(2.0 / math.pi)
LAST = (((1,), (1,)), ((), ()))
FIRST = (((0,), (0,)), ((), ()))
F32 = jnp.float32
BF16 = jnp.bfloat16
MESH = pl.DeviceIdType.MESH


W = 128
RB = 1024
PHI = 8
AHEAD = 8
SLOTS = 8


def gelu_parts(c):
    c2 = c * c
    t = jnp.tanh(SQRT_TWO_PI * (c * (1.0 + GELU_COEF * c2)))
    half = 0.5 * (1.0 + t)
    slope = half + 0.5 * c * (1.0 - t * t) * SQRT_TWO_PI * (1.0 + 3.0 * GELU_COEF * c2)
    return c * half, slope


def hidden_kernel(x_in, up, down, z_in,
                  h_out, dc_own, dc_oth, x_out, z_own, z_oth, dx_own, dx_part, dx_got, dcp_own, dcp_oth, up_y, up_yd, up_d, up_x, up_xd, down_d, down_x, down_xd,
                  xv, zv, uv, vv, acc, h_st, dc_st,
                  act_send, act_recv, wx_send, wx_recv, wd_send, wd_recv, all_send, all_recv,
                  load_sem, local_sem, out_sem, extra_sem):
    cz, cy, cx = lax.axis_index("cz"), lax.axis_index("cy"), lax.axis_index("cx")
    to_x, to_y, to_d = {"cy": 1 - cy}, {"cz": 1 - cz}, {"cx": 1 - cx}
    rows, dk = x_in.shape
    ffc = up.shape[1]
    dq = down.shape[1]
    chunks = ffc // W

    def remote(src, dst, send, recv, dev):
        return pltpu.make_async_remote_copy(src_ref=src, dst_ref=dst, send_sem=send, recv_sem=recv,
                                            device_id=dev, device_id_type=MESH)

    def mine(c):
        return pl.ds(pl.multiple_of(c * W, W), W)

    def frow(f, c):
        return pl.ds(pl.multiple_of(f * ffc + c * W, W), W)

    own, oth = pl.ds(0, rows), pl.ds(rows, rows)
    near, far = pl.ds(0, dk), pl.ds(dk, dk)

    x1 = remote(x_in, xv.at[own, far], act_send.at[0], act_recv.at[0], to_x)
    z1 = remote(z_in, zv.at[own, far], act_send.at[1], act_recv.at[1], to_x)
    x2 = remote(x_in, xv.at[oth, near], act_send.at[2], act_recv.at[2], to_y)
    z2 = remote(z_in, zv.at[oth, near], act_send.at[3], act_recv.at[3], to_y)
    x3 = remote(xv.at[own, far], xv.at[oth, far], act_send.at[4], act_recv.at[4], to_y)
    z3 = remote(zv.at[own, far], zv.at[oth, far], act_send.at[5], act_recv.at[5], to_y)
    up_all = remote(up, up_d, all_send.at[0], all_recv.at[0], to_d)
    down_all = remote(down, down_d, all_send.at[1], all_recv.at[1], to_d)

    split = chunks - PHI
    tail = pl.ds(split * W, PHI * W)
    up_tail = remote(up.at[:, tail], up_y, all_send.at[2], all_recv.at[2], to_y)
    up_tail_d = remote(up_y, up_yd, all_send.at[3], all_recv.at[3], to_d)
    part_save = pltpu.make_async_copy(acc.at[oth], dx_part, local_sem.at[3])
    part_send = remote(dx_part, dx_got, all_send.at[4], all_recv.at[4], to_y)
    own_save = pltpu.make_async_copy(acc.at[own], dx_own, local_sem.at[4])

    def over_x(c):
        return [remote(up.at[:, mine(c)], up_x.at[:, mine(c)], wx_send.at[c, 0], wx_recv.at[c, 0], to_x)] + [
            remote(down.at[frow(f, c)], down_x.at[frow(f, c)], wx_send.at[c, 1 + f], wx_recv.at[c, 1 + f], to_x)
            for f in range(2)]

    def over_d(c):
        return [remote(up_x.at[:, mine(c)], up_xd.at[:, mine(c)], wd_send.at[c, 0], wd_recv.at[c, 0], to_d)] + [
            remote(down_x.at[frow(f, c)], down_xd.at[frow(f, c)], wd_send.at[c, 1 + f], wd_recv.at[c, 1 + f], to_d)
            for f in range(2)]

    def lanes(part, core):
        return pl.ds(pl.multiple_of(part * dk + core * dq, 128), dq)

    def loads(c, late):
        slot = lax.rem(c, SLOTS)
        left, right = pl.ds(0, W), pl.ds(W, W)
        if late:
            moves = [(up_xd.at[:, mine(c)], uv.at[slot, far, right])]
            parts = [(down_xd, lanes(1, 1 - cx))]
        else:
            moves = [(up.at[:, mine(c)], uv.at[slot, near, left]),
                     (up_d.at[:, mine(c)], uv.at[slot, near, right]),
                     (up_x.at[:, mine(c)], uv.at[slot, far, left])]
            parts = [(down, lanes(0, cx)), (down_d, lanes(0, 1 - cx)), (down_x, lanes(1, cx))]
        for src, lane in parts:
            moves.append((src.at[frow(cx, c)], vv.at[slot, left, lane]))
            moves.append((src.at[frow(1 - cx, c)], vv.at[slot, right, lane]))
        base = 9 if late else 0
        return [pltpu.make_async_copy(s, d, load_sem.at[base + i]) for i, (s, d) in enumerate(moves)]

    barrier = pltpu.get_barrier_semaphore()
    for dev in (to_x, to_y, to_d):
        pl.semaphore_signal(barrier, inc=1, device_id=dev, device_id_type=MESH)
    pl.semaphore_wait(barrier, 3)

    x1.start()
    x2.start()
    z1.start()
    z2.start()
    for c in range(AHEAD):
        for copy in over_x(c):
            copy.start()
    up_all.start()
    down_all.start()
    x0 = pltpu.make_async_copy(x_in, xv.at[own, near], local_sem.at[0])
    z0 = pltpu.make_async_copy(z_in, zv.at[own, near], local_sem.at[1])
    x0.start()
    z0.start()

    @pl.loop(0, 2 * rows // 256)
    def _(i):
        acc[pl.ds(pl.multiple_of(i * 256, 256), 256), :] = jnp.zeros((256, dk), F32)

    x1.wait_recv()
    x3.start()
    z1.wait_recv()
    z3.start()
    up_tail.start()
    x0.wait()
    z0.wait()
    up_all.wait_recv()
    down_all.wait_recv()
    x_save = pltpu.make_async_copy(xv.at[:, near], x_out, local_sem.at[0])
    z_save = [pltpu.make_async_copy(zv.at[:, lanes(0, cx)], z_own, local_sem.at[1]),
              pltpu.make_async_copy(zv.at[:, lanes(0, 1 - cx)], z_oth, local_sem.at[2])]

    def outs(n, c, r0):
        sl = lax.rem(n, 2)
        r = pl.ds(r0, RB)
        left, right = pl.ds(0, W), pl.ds(W, W)
        moves = ((h_st.at[sl, :, left], h_out.at[r, frow(cx, c)]), (h_st.at[sl, :, right], h_out.at[r, frow(1 - cx, c)]),
                 (dc_st.at[sl, :, left], dc_own.at[r, mine(c)]), (dc_st.at[sl, :, right], dc_oth.at[r, mine(c)]))
        return [pltpu.make_async_copy(src, dst, out_sem.at[sl, i]) for i, (src, dst) in enumerate(moves)]

    def extra(n, c):
        sl = lax.rem(n, 2)
        cols = pl.ds(pl.multiple_of((c - split) * W, W), W)
        return [pltpu.make_async_copy(dc_st.at[sl, :, pl.ds(0, W)], dcp_own.at[:, cols], extra_sem.at[0]),
                pltpu.make_async_copy(dc_st.at[sl, :, pl.ds(W, W)], dcp_oth.at[:, cols], extra_sem.at[1])]

    steps = 2 * chunks

    @pl.loop(0, steps)
    def _(s):
        late = s >= 2 * SLOTS
        c = jnp.where(late, SLOTS + (s - 2 * SLOTS) // 2, lax.rem(s, SLOTS))
        half = jnp.where(late, jnp.where(c < split, 1 - lax.rem(s, 2), lax.rem(s, 2)), s // SLOTS)
        odd = lax.rem(s, 2) == 1
        hc = jnp.where(s < SLOTS, s, SLOTS + (s - 2 * SLOTS + 1) // 2)

        @pl.when(s == 2 * split - 1)
        def _():
            part_save.start()
            up_tail.wait_recv()
            up_tail_d.start()
            part_save.wait()
            part_send.start()

        @pl.when((s < SLOTS) | ((s >= 2 * SLOTS - 1) & odd & (s < steps - 1)))
        def _():
            for copy in over_x(hc):
                copy.wait_recv()
            for copy in over_d(hc):
                copy.start()

            @pl.when(hc + AHEAD < chunks)
            def _():
                for copy in over_x(hc + AHEAD):
                    copy.start()

            for copy in loads(hc, False):
                copy.start()

        @pl.when((s < SLOTS) | (late & ~odd))
        def _():
            for copy in over_d(c):
                copy.wait_recv()
            for copy in loads(c, True):
                copy.start()
            for copy in loads(c, False) + loads(c, True):
                copy.wait()

        @pl.when(s == SLOTS)
        def _():
            x2.wait_recv()
            z2.wait_recv()
            x_save.start()
            for copy in z_save:
                copy.start()
            x3.wait_recv()
            z3.wait_recv()

        @pl.when(s == steps - 1)
        def _():
            own_save.start()

        slot = lax.rem(c, SLOTS)
        r0 = pl.multiple_of(half * rows, RB)
        sl = lax.rem(s, 2)
        cc = jnp.dot(xv[pl.ds(r0, RB), :], uv[slot], preferred_element_type=F32)
        dh = lax.dot_general(zv[pl.ds(r0, RB), :], vv[slot], LAST, preferred_element_type=F32)
        h, slope = gelu_parts(cc.astype(BF16).astype(F32))
        dc = (dh * slope).astype(BF16)

        @pl.when(s >= 2)
        def _():
            for copy in outs(s, c, r0):
                copy.wait()

        @pl.when((s >= 2 * split + 3) & odd)
        def _():
            for copy in extra(s, c):
                copy.wait()

        h_st[sl] = h.astype(BF16)
        dc_st[sl] = dc
        for copy in outs(s, c, r0):
            copy.start()

        @pl.when((half == 0) | (c < split))
        def _():
            acc[pl.ds(r0, RB), :] += lax.dot_general(dc_st[sl], uv[slot, near, :], LAST, preferred_element_type=F32)

        @pl.when((half == 1) & (c >= split))
        def _():
            for copy in extra(s, c):
                copy.start()

    for n in range(2):
        for copy in outs(n, 0, 0):
            copy.wait()
    for copy in extra(1, split):
        copy.wait()
    own_save.wait()
    up_tail_d.wait_recv()
    part_send.wait_recv()
    x_save.wait()
    for copy in z_save:
        copy.wait()
    for copy in (x1, z1, x2, z2, x3, z3, up_all, down_all, up_tail, up_tail_d, part_send):
        copy.wait_send()

    @pl.loop(0, chunks)
    def _(c):
        for copy in over_x(c) + over_d(c):
            copy.wait_send()


def hidden_call(x_act, w_up, w_down, z_grad):
    rows, dk = x_act.shape
    ffc = w_up.shape[1]
    ff, dq = w_down.shape
    chunks = ffc // W
    flops = 2 * rows * 2 * ff * dk * 5
    hbm = pl.BlockSpec(memory_space=pl.ANY)
    sds = jax.ShapeDtypeStruct
    out_shape = [
        sds((2 * rows, ff), BF16), sds((2 * rows, ffc), BF16), sds((2 * rows, ffc), BF16),
        sds((2 * rows, dk), BF16), sds((2 * rows, dq), BF16), sds((2 * rows, dq), BF16),
        sds((rows, dk), F32), sds((rows, dk), F32), sds((rows, dk), F32),
        sds((rows, PHI * W), BF16), sds((rows, PHI * W), BF16), sds((dk, PHI * W), BF16), sds((dk, PHI * W), BF16),
        sds(w_up.shape, BF16), sds(w_up.shape, BF16), sds(w_up.shape, BF16),
        sds(w_down.shape, BF16), sds(w_down.shape, BF16), sds(w_down.shape, BF16),
    ]
    dma = pltpu.SemaphoreType.DMA
    return pl.pallas_call(
        hidden_kernel,
        in_specs=[hbm] * 4,
        out_specs=[hbm] * len(out_shape),
        out_shape=out_shape,
        scratch_shapes=[
            pltpu.VMEM((2 * rows, 2 * dk), BF16), pltpu.VMEM((2 * rows, 2 * dk), BF16),
            pltpu.VMEM((SLOTS, 2 * dk, 2 * W), BF16), pltpu.VMEM((SLOTS, 2 * W, 2 * dk), BF16),
            pltpu.VMEM((2 * rows, dk), F32),
            pltpu.VMEM((2, RB, 2 * W), BF16), pltpu.VMEM((2, RB, 2 * W), BF16),
            dma((6,)), dma((6,)), dma((chunks, 3)), dma((chunks, 3)), dma((chunks, 3)), dma((chunks, 3)),
            dma((5,)), dma((5,)), dma((12,)), dma((5,)), dma((2, 4)), dma((2,)),
        ],
        compiler_params=pltpu.CompilerParams(
            collective_id=0, has_side_effects=True, vmem_limit_bytes=67_000_000),
        cost_estimate=pl.CostEstimate(flops=flops, bytes_accessed=200_000_000, transcendentals=2 * rows * ff),
        name="hidden",
    )(x_act, w_up, w_down, z_grad)


def solution(mesh):
    row_spec = P(("dp", "cx", "cz"), "cy")
    up_spec = P("cy", ("cz", "cx"))
    down_spec = P("cz", ("cy", "cx"))
    up_out = P(("dp", "cy"), ("cz", "cx"))
    down_out = P(("dp", "cz"), ("cy", "cx"))
    swap = [(0, 1), (1, 0)]

    def local_step(x_act, w_up, w_down, z_grad):
        (h, dc_own, dc_oth, xs, z_own, z_oth, dx_own, _, dx_got, dcp_own, dcp_oth, up_y, up_yd) = hidden_call(
            x_act, w_up, w_down, z_grad)[:13]
        dcr_own = lax.ppermute(dcp_own, "cz", swap)
        dcr_oth = lax.ppermute(dcp_oth, "cz", swap)
        down_part = lax.dot_general(h, z_oth, FIRST, preferred_element_type=F32)
        up_part = lax.dot_general(xs, dc_oth, FIRST, preferred_element_type=F32)
        down_got = lax.ppermute(down_part, "cx", swap)
        up_got = lax.ppermute(up_part, "cx", swap)
        down_grad = (lax.dot_general(h, z_own, FIRST, preferred_element_type=F32) + down_got).astype(BF16)
        up_grad = (lax.dot_general(xs, dc_own, FIRST, preferred_element_type=F32) + up_got).astype(BF16)
        dx = lax.dot_general(dcr_own, up_y, LAST, preferred_element_type=F32) + (dx_own + dx_got)
        x_grad = (lax.dot_general(dcr_oth, up_yd, LAST, preferred_element_type=F32) + dx).astype(BF16)
        return (x_grad, up_grad, down_grad)

    return jax.shard_map(local_step, mesh=mesh, in_specs=(row_spec, up_spec, down_spec, row_spec), out_specs=(row_spec, up_out, down_out), check_vma=False)
```

```python
import math
import jax
import jax.numpy as jnp
from jax import lax
from jax.experimental import pallas as pl
from jax.experimental.pallas import tpu as pltpu
from jax.sharding import PartitionSpec as P

GELU_COEF = 0.044715
SQRT_TWO_PI = math.sqrt(2.0 / math.pi)
LAST = (((1,), (1,)), ((), ()))
FIRST = (((0,), (0,)), ((), ()))
F32 = jnp.float32
BF16 = jnp.bfloat16
MESH = pl.DeviceIdType.MESH


W = 128
RB = 1024
PHI = 8
AHEAD = 8
SLOTS = 8


def gelu_parts(c):
    c2 = c * c
    t = jnp.tanh(SQRT_TWO_PI * (c * (1.0 + GELU_COEF * c2)))
    half = 0.5 * (1.0 + t)
    slope = half + 0.5 * c * (1.0 - t * t) * SQRT_TWO_PI * (1.0 + 3.0 * GELU_COEF * c2)
    return c * half, slope


def hidden_kernel(x_in, up, down, z_in,
                  h_out, dc_out, x_out, z_out, dx_own, dx_part, dx_got, dcp_own, dcp_oth, up_y, up_yd, up_d, up_x, up_xd, down_d, down_x, down_xd,
                  xv, zv, uv, vv, acc, h_st, dc_st,
                  act_send, act_recv, wx_send, wx_recv, wd_send, wd_recv, all_send, all_recv,
                  load_sem, local_sem, out_sem, extra_sem, push_send, push_recv):
    cz, cy, cx = lax.axis_index("cz"), lax.axis_index("cy"), lax.axis_index("cx")
    to_x, to_y, to_d = {"cy": 1 - cy}, {"cz": 1 - cz}, {"cx": 1 - cx}
    rows, dk = x_in.shape
    ffc = up.shape[1]
    dq = down.shape[1]
    chunks = ffc // W

    def remote(src, dst, send, recv, dev):
        return pltpu.make_async_remote_copy(src_ref=src, dst_ref=dst, send_sem=send, recv_sem=recv,
                                            device_id=dev, device_id_type=MESH)

    def mine(c):
        return pl.ds(pl.multiple_of(c * W, W), W)

    def frow(f, c):
        return pl.ds(pl.multiple_of(f * ffc + c * W, W), W)

    own, oth = pl.ds(0, rows), pl.ds(rows, rows)
    near, far = pl.ds(0, dk), pl.ds(dk, dk)

    x1 = remote(x_in, xv.at[own, far], act_send.at[0], act_recv.at[0], to_x)
    z1 = remote(z_in, zv.at[own, far], act_send.at[1], act_recv.at[1], to_x)
    x2 = remote(x_in, xv.at[oth, near], act_send.at[2], act_recv.at[2], to_y)
    z2 = remote(z_in, zv.at[oth, near], act_send.at[3], act_recv.at[3], to_y)
    x3 = remote(xv.at[own, far], xv.at[oth, far], act_send.at[4], act_recv.at[4], to_y)
    z3 = remote(zv.at[own, far], zv.at[oth, far], act_send.at[5], act_recv.at[5], to_y)
    up_all = remote(up, up_d, all_send.at[0], all_recv.at[0], to_d)
    down_all = remote(down, down_d, all_send.at[1], all_recv.at[1], to_d)

    split = chunks - PHI
    tail = pl.ds(split * W, PHI * W)
    up_tail = remote(up.at[:, tail], up_y, all_send.at[2], all_recv.at[2], to_y)
    up_tail_d = remote(up_y, up_yd, all_send.at[3], all_recv.at[3], to_d)
    part_save = pltpu.make_async_copy(acc.at[oth], dx_part, local_sem.at[3])
    part_send = remote(dx_part, dx_got, all_send.at[4], all_recv.at[4], to_y)
    own_save = pltpu.make_async_copy(acc.at[own], dx_own, local_sem.at[4])

    def over_x(c):
        return [remote(up.at[:, mine(c)], up_x.at[:, mine(c)], wx_send.at[c, 0], wx_recv.at[c, 0], to_x)] + [
            remote(down.at[frow(f, c)], down_x.at[frow(f, c)], wx_send.at[c, 1 + f], wx_recv.at[c, 1 + f], to_x)
            for f in range(2)]

    def over_d(c):
        return [remote(up_x.at[:, mine(c)], up_xd.at[:, mine(c)], wd_send.at[c, 0], wd_recv.at[c, 0], to_d)] + [
            remote(down_x.at[frow(f, c)], down_xd.at[frow(f, c)], wd_send.at[c, 1 + f], wd_recv.at[c, 1 + f], to_d)
            for f in range(2)]

    def lanes(part, core):
        return pl.ds(pl.multiple_of(part * dk + core * dq, 128), dq)

    def loads(c, late):
        slot = lax.rem(c, SLOTS)
        left, right = pl.ds(0, W), pl.ds(W, W)
        if late:
            moves = [(up_xd.at[:, mine(c)], uv.at[slot, far, right])]
            parts = [(down_xd, lanes(1, 1 - cx))]
        else:
            moves = [(up.at[:, mine(c)], uv.at[slot, near, left]),
                     (up_d.at[:, mine(c)], uv.at[slot, near, right]),
                     (up_x.at[:, mine(c)], uv.at[slot, far, left])]
            parts = [(down, lanes(0, cx)), (down_d, lanes(0, 1 - cx)), (down_x, lanes(1, cx))]
        for src, lane in parts:
            moves.append((src.at[frow(cx, c)], vv.at[slot, left, lane]))
            moves.append((src.at[frow(1 - cx, c)], vv.at[slot, right, lane]))
        base = 9 if late else 0
        return [pltpu.make_async_copy(s, d, load_sem.at[base + i]) for i, (s, d) in enumerate(moves)]

    barrier = pltpu.get_barrier_semaphore()
    for dev in (to_x, to_y, to_d):
        pl.semaphore_signal(barrier, inc=1, device_id=dev, device_id_type=MESH)
    pl.semaphore_wait(barrier, 3)

    x1.start()
    x2.start()
    z1.start()
    z2.start()
    for c in range(AHEAD):
        for copy in over_x(c):
            copy.start()
    up_all.start()
    down_all.start()
    x0 = pltpu.make_async_copy(x_in, xv.at[own, near], local_sem.at[0])
    z0 = pltpu.make_async_copy(z_in, zv.at[own, near], local_sem.at[1])
    x0.start()
    z0.start()

    @pl.loop(0, 2 * rows // 256)
    def _(i):
        acc[pl.ds(pl.multiple_of(i * 256, 256), 256), :] = jnp.zeros((256, dk), F32)

    x1.wait_recv()
    x3.start()
    z1.wait_recv()
    z3.start()
    up_tail.start()
    x0.wait()
    z0.wait()
    up_all.wait_recv()
    down_all.wait_recv()
    mine_all, core_all = pl.ds(0, 2 * rows), pl.ds(2 * rows, 2 * rows)
    saves = [pltpu.make_async_copy(xv.at[:, near], x_out.at[mine_all], local_sem.at[0]),
             pltpu.make_async_copy(zv.at[:, lanes(0, cx)], z_out.at[mine_all], local_sem.at[1])]
    shares = [remote(xv.at[:, near], x_out.at[core_all], all_send.at[5], all_recv.at[5], to_d),
              remote(zv.at[:, lanes(0, 1 - cx)], z_out.at[core_all], all_send.at[6], all_recv.at[6], to_d)]

    def outs(n, c, r0):
        sl = lax.rem(n, 2)
        r = pl.ds(r0, RB)
        left, right = pl.ds(0, W), pl.ds(W, W)
        far_r = pl.ds(2 * rows + r0, RB)
        moves = ((h_st.at[sl, :, left], h_out.at[r, frow(cx, c)]), (h_st.at[sl, :, right], h_out.at[r, frow(1 - cx, c)]),
                 (dc_st.at[sl, :, left], dc_out.at[r, mine(c)]))
        pushes = ((h_st.at[sl, :, left], h_out.at[far_r, frow(cx, c)]), (h_st.at[sl, :, right], h_out.at[far_r, frow(1 - cx, c)]),
                  (dc_st.at[sl, :, right], dc_out.at[far_r, mine(c)]))
        return ([pltpu.make_async_copy(src, dst, out_sem.at[sl, i]) for i, (src, dst) in enumerate(moves)],
                [remote(src, dst, push_send.at[sl, i], push_recv.at[n, i], to_d) for i, (src, dst) in enumerate(pushes)])

    def extra(n, c):
        sl = lax.rem(n, 2)
        cols = pl.ds(pl.multiple_of((c - split) * W, W), W)
        return [pltpu.make_async_copy(dc_st.at[sl, :, pl.ds(0, W)], dcp_own.at[:, cols], extra_sem.at[0]),
                pltpu.make_async_copy(dc_st.at[sl, :, pl.ds(W, W)], dcp_oth.at[:, cols], extra_sem.at[1])]

    steps = 2 * chunks

    def drain(first, last):
        @pl.loop(first, last)
        def _(c):
            for copy in over_x(c) + over_d(c):
                copy.wait_send()

    @pl.loop(0, steps)
    def _(s):
        late = s >= 2 * SLOTS
        c = jnp.where(late, SLOTS + (s - 2 * SLOTS) // 2, lax.rem(s, SLOTS))
        half = jnp.where(late, jnp.where(c < split, 1 - lax.rem(s, 2), lax.rem(s, 2)), s // SLOTS)
        odd = lax.rem(s, 2) == 1
        hc = jnp.where(s < SLOTS, s, SLOTS + (s - 2 * SLOTS + 1) // 2)

        @pl.when(s == 2 * split - 1)
        def _():
            part_save.start()
            up_tail.wait_recv()
            up_tail_d.start()
            part_save.wait()
            part_send.start()

        @pl.when((s < SLOTS) | ((s >= 2 * SLOTS - 1) & odd & (s < steps - 1)))
        def _():
            for copy in over_x(hc):
                copy.wait_recv()
            for copy in over_d(hc):
                copy.start()

            @pl.when(hc + AHEAD < chunks)
            def _():
                for copy in over_x(hc + AHEAD):
                    copy.start()

            for copy in loads(hc, False):
                copy.start()

        @pl.when((s < SLOTS) | (late & ~odd))
        def _():
            @pl.when(s < SLOTS)
            def _():
                for copy in over_d(c):
                    copy.wait_recv()
                for copy in loads(c, True):
                    copy.start()

            for copy in loads(c, False) + loads(c, True):
                copy.wait()

        @pl.when(s == SLOTS)
        def _():
            x2.wait_recv()
            z2.wait_recv()
            for copy in saves + shares:
                copy.start()
            x3.wait_recv()
            z3.wait_recv()

        @pl.when(s == steps - 4)
        def _():
            for copy in saves:
                copy.wait()
            for copy in shares:
                copy.wait_send()
                copy.wait_recv()
            up_tail_d.wait_recv()
            for copy in (x1, z1, x2, z2, x3, z3, up_all, down_all, up_tail, up_tail_d):
                copy.wait_send()
            drain(0, chunks - 4)

        @pl.when(s == steps - 1)
        def _():
            own_save.start()

        slot = lax.rem(c, SLOTS)
        r0 = pl.multiple_of(half * rows, RB)
        sl = lax.rem(s, 2)
        cc = jnp.dot(xv[pl.ds(r0, RB), :], uv[slot], preferred_element_type=F32)
        dh = lax.dot_general(zv[pl.ds(r0, RB), :], vv[slot], LAST, preferred_element_type=F32)
        h, slope = gelu_parts(cc.astype(BF16).astype(F32))
        dc = (dh * slope).astype(BF16)

        @pl.when(s >= 2)
        def _():
            keep, push = outs(s - 2, c, r0)
            for copy in keep:
                copy.wait()
            for copy in push:
                copy.wait_send()
                copy.wait_recv()

        @pl.when((s >= 2 * split + 3) & odd)
        def _():
            for copy in extra(s, c):
                copy.wait()

        h_st[sl] = h.astype(BF16)
        dc_st[sl] = dc

        @pl.when((s >= 2 * SLOTS - 1) & odd & (s < steps - 1))
        def _():
            for copy in over_d(hc):
                copy.wait_recv()
            for copy in loads(hc, True):
                copy.start()

        @pl.when((half == 0) | (c < split))
        def _():
            acc[pl.ds(r0, RB), :] += lax.dot_general(dc_st[sl], uv[slot, near, :], LAST, preferred_element_type=F32)

        keep, push = outs(s, c, r0)
        for copy in keep + push:
            copy.start()

        @pl.when((half == 1) & (c >= split))
        def _():
            for copy in extra(s, c):
                copy.start()

    for n in range(2):
        keep, push = outs(steps - 2 + n, 0, 0)
        for copy in keep:
            copy.wait()
        for copy in push:
            copy.wait_send()
            copy.wait_recv()
    for copy in extra(1, split):
        copy.wait()
    own_save.wait()
    part_send.wait_recv()
    part_send.wait_send()
    drain(chunks - 4, chunks)


def hidden_call(x_act, w_up, w_down, z_grad):
    rows, dk = x_act.shape
    ffc = w_up.shape[1]
    ff, dq = w_down.shape
    chunks = ffc // W
    flops = 2 * rows * 2 * ff * dk * 5
    hbm = pl.BlockSpec(memory_space=pl.ANY)
    sds = jax.ShapeDtypeStruct
    out_shape = [
        sds((4 * rows, ff), BF16), sds((4 * rows, ffc), BF16), sds((4 * rows, dk), BF16), sds((4 * rows, dq), BF16),
        sds((rows, dk), F32), sds((rows, dk), F32), sds((rows, dk), F32),
        sds((rows, PHI * W), BF16), sds((rows, PHI * W), BF16), sds((dk, PHI * W), BF16), sds((dk, PHI * W), BF16),
        sds(w_up.shape, BF16), sds(w_up.shape, BF16), sds(w_up.shape, BF16),
        sds(w_down.shape, BF16), sds(w_down.shape, BF16), sds(w_down.shape, BF16),
    ]
    dma = pltpu.SemaphoreType.DMA
    return pl.pallas_call(
        hidden_kernel,
        in_specs=[hbm] * 4,
        out_specs=[hbm] * len(out_shape),
        out_shape=out_shape,
        scratch_shapes=[
            pltpu.VMEM((2 * rows, 2 * dk), BF16), pltpu.VMEM((2 * rows, 2 * dk), BF16),
            pltpu.VMEM((SLOTS, 2 * dk, 2 * W), BF16), pltpu.VMEM((SLOTS, 2 * W, 2 * dk), BF16),
            pltpu.VMEM((2 * rows, dk), F32),
            pltpu.VMEM((2, RB, 2 * W), BF16), pltpu.VMEM((2, RB, 2 * W), BF16),
            dma((6,)), dma((6,)), dma((chunks, 3)), dma((chunks, 3)), dma((chunks, 3)), dma((chunks, 3)),
            dma((7,)), dma((7,)), dma((12,)), dma((5,)), dma((2, 3)), dma((2,)), dma((2, 3)), dma((4 * ffc // (2 * W), 3)),
        ],
        compiler_params=pltpu.CompilerParams(
            collective_id=0, has_side_effects=True, vmem_limit_bytes=67_000_000),
        cost_estimate=pl.CostEstimate(flops=flops, bytes_accessed=200_000_000, transcendentals=2 * rows * ff),
        name="hidden",
    )(x_act, w_up, w_down, z_grad)


def solution(mesh):
    row_spec = P(("dp", "cx", "cz"), "cy")
    up_spec = P("cy", ("cz", "cx"))
    down_spec = P("cz", ("cy", "cx"))
    up_out = P(("dp", "cy"), ("cz", "cx"))
    down_out = P(("dp", "cz"), ("cy", "cx"))
    swap = [(0, 1), (1, 0)]

    def local_step(x_act, w_up, w_down, z_grad):
        h, dc, xs, zs, dx_own, _, dx_got, dcp_own, dcp_oth, up_y, up_yd = hidden_call(x_act, w_up, w_down, z_grad)[:11]
        dcr_own = lax.ppermute(dcp_own, "cz", swap)
        dcr_oth = lax.ppermute(dcp_oth, "cz", swap)
        down_grad = lax.dot_general(h, zs, FIRST, preferred_element_type=F32).astype(BF16)
        up_grad = lax.dot_general(xs, dc, FIRST, preferred_element_type=F32).astype(BF16)
        dx = lax.dot_general(dcr_own, up_y, LAST, preferred_element_type=F32) + (dx_own + dx_got)
        x_grad = (lax.dot_general(dcr_oth, up_yd, LAST, preferred_element_type=F32) + dx).astype(BF16)
        return (x_grad, up_grad, down_grad)

    return jax.shard_map(local_step, mesh=mesh, in_specs=(row_spec, up_spec, down_spec, row_spec), out_specs=(row_spec, up_out, down_out), check_vma=False)
```

```python
import math
import jax
import jax.numpy as jnp
from jax import lax
from jax.experimental import pallas as pl
from jax.experimental.pallas import tpu as pltpu
from jax.sharding import PartitionSpec as P

GELU_COEF = 0.044715
SQRT_TWO_PI = math.sqrt(2.0 / math.pi)
LAST = (((1,), (1,)), ((), ()))
FIRST = (((0,), (0,)), ((), ()))
F32 = jnp.float32
BF16 = jnp.bfloat16
MESH = pl.DeviceIdType.MESH


W = 128
RB = 1024
PHI = 8
AHEAD = 8
SLOTS = 8


def gelu_parts(c):
    c2 = c * c
    t = jnp.tanh(SQRT_TWO_PI * (c * (1.0 + GELU_COEF * c2)))
    half = 0.5 * (1.0 + t)
    slope = half + 0.5 * c * (1.0 - t * t) * SQRT_TWO_PI * (1.0 + 3.0 * GELU_COEF * c2)
    return c * half, slope


def hidden_kernel(x_in, up, down, z_in,
                  h_out, dc_out, x_out, z_out, dx_own, dx_part, dx_got, dcp_own, dcp_oth, up_y, up_yd, up_d, up_x, up_xd, down_d, down_x, down_xd,
                  xv, zv, uv, vv, acc, h_st, dc_st,
                  act_send, act_recv, wx_send, wx_recv, wd_send, wd_recv, all_send, all_recv,
                  load_sem, local_sem, out_sem, extra_sem, push_send, push_recv):
    cz, cy, cx = lax.axis_index("cz"), lax.axis_index("cy"), lax.axis_index("cx")
    to_x, to_y, to_d = {"cy": 1 - cy}, {"cz": 1 - cz}, {"cx": 1 - cx}
    rows, dk = x_in.shape
    ffc = up.shape[1]
    dq = down.shape[1]
    chunks = ffc // W

    def remote(src, dst, send, recv, dev):
        return pltpu.make_async_remote_copy(src_ref=src, dst_ref=dst, send_sem=send, recv_sem=recv,
                                            device_id=dev, device_id_type=MESH)

    def mine(c):
        return pl.ds(pl.multiple_of(c * W, W), W)

    def frow(f, c):
        return pl.ds(pl.multiple_of(f * ffc + c * W, W), W)

    own, oth = pl.ds(0, rows), pl.ds(rows, rows)
    near, far = pl.ds(0, dk), pl.ds(dk, dk)

    x1 = remote(x_in, xv.at[own, far], act_send.at[0], act_recv.at[0], to_x)
    z1 = remote(z_in, zv.at[own, far], act_send.at[1], act_recv.at[1], to_x)
    x2 = remote(x_in, xv.at[oth, near], act_send.at[2], act_recv.at[2], to_y)
    z2 = remote(z_in, zv.at[oth, near], act_send.at[3], act_recv.at[3], to_y)
    x3 = remote(xv.at[own, far], xv.at[oth, far], act_send.at[4], act_recv.at[4], to_y)
    z3 = remote(zv.at[own, far], zv.at[oth, far], act_send.at[5], act_recv.at[5], to_y)
    up_all = remote(up, up_d, all_send.at[0], all_recv.at[0], to_d)
    down_all = remote(down, down_d, all_send.at[1], all_recv.at[1], to_d)

    split = chunks - PHI
    tail = pl.ds(split * W, PHI * W)
    up_tail = remote(up.at[:, tail], up_y, all_send.at[2], all_recv.at[2], to_y)
    up_tail_d = remote(up_y, up_yd, all_send.at[3], all_recv.at[3], to_d)
    part_save = pltpu.make_async_copy(acc.at[oth], dx_part, local_sem.at[3])
    part_send = remote(dx_part, dx_got, all_send.at[4], all_recv.at[4], to_y)
    own_save = pltpu.make_async_copy(acc.at[own], dx_own, local_sem.at[4])

    def over_x(c):
        return [remote(up.at[:, mine(c)], up_x.at[:, mine(c)], wx_send.at[c, 0], wx_recv.at[c, 0], to_x)] + [
            remote(down.at[frow(f, c)], down_x.at[frow(f, c)], wx_send.at[c, 1 + f], wx_recv.at[c, 1 + f], to_x)
            for f in range(2)]

    def over_d(c):
        return [remote(up_x.at[:, mine(c)], up_xd.at[:, mine(c)], wd_send.at[c, 0], wd_recv.at[c, 0], to_d)] + [
            remote(down_x.at[frow(f, c)], down_xd.at[frow(f, c)], wd_send.at[c, 1 + f], wd_recv.at[c, 1 + f], to_d)
            for f in range(2)]

    def lanes(part, core):
        return pl.ds(pl.multiple_of(part * dk + core * dq, 128), dq)

    def loads(c, late):
        slot = lax.rem(c, SLOTS)
        left, right = pl.ds(0, W), pl.ds(W, W)
        if late:
            moves = [(up_xd.at[:, mine(c)], uv.at[slot, far, right])]
            parts = [(down_xd, lanes(1, 1 - cx))]
        else:
            moves = [(up.at[:, mine(c)], uv.at[slot, near, left]),
                     (up_d.at[:, mine(c)], uv.at[slot, near, right]),
                     (up_x.at[:, mine(c)], uv.at[slot, far, left])]
            parts = [(down, lanes(0, cx)), (down_d, lanes(0, 1 - cx)), (down_x, lanes(1, cx))]
        for src, lane in parts:
            moves.append((src.at[frow(cx, c)], vv.at[slot, left, lane]))
            moves.append((src.at[frow(1 - cx, c)], vv.at[slot, right, lane]))
        base = 9 if late else 0
        return [pltpu.make_async_copy(s, d, load_sem.at[base + i]) for i, (s, d) in enumerate(moves)]

    barrier = pltpu.get_barrier_semaphore()
    for dev in (to_x, to_y, to_d):
        pl.semaphore_signal(barrier, inc=1, device_id=dev, device_id_type=MESH)
    pl.semaphore_wait(barrier, 3)

    x1.start()
    x2.start()
    z1.start()
    z2.start()
    for c in range(AHEAD):
        for copy in over_x(c):
            copy.start()
    up_all.start()
    down_all.start()
    x0 = pltpu.make_async_copy(x_in, xv.at[own, near], local_sem.at[0])
    z0 = pltpu.make_async_copy(z_in, zv.at[own, near], local_sem.at[1])
    x0.start()
    z0.start()

    @pl.loop(0, 2 * rows // 256)
    def _(i):
        acc[pl.ds(pl.multiple_of(i * 256, 256), 256), :] = jnp.zeros((256, dk), F32)

    x1.wait_recv()
    x3.start()
    z1.wait_recv()
    z3.start()
    up_tail.start()
    x0.wait()
    z0.wait()
    up_all.wait_recv()
    down_all.wait_recv()
    mine_all, core_all = pl.ds(0, 2 * rows), pl.ds(2 * rows, 2 * rows)
    saves = [pltpu.make_async_copy(xv.at[:, near], x_out.at[mine_all], local_sem.at[0]),
             pltpu.make_async_copy(zv.at[:, lanes(0, cx)], z_out.at[mine_all], local_sem.at[1])]
    shares = [remote(xv.at[:, near], x_out.at[core_all], all_send.at[5], all_recv.at[5], to_d),
              remote(zv.at[:, lanes(0, 1 - cx)], z_out.at[core_all], all_send.at[6], all_recv.at[6], to_d)]

    def outs(n, c, r0):
        sl = lax.rem(n, 2)
        r = pl.ds(r0, RB)
        left, right = pl.ds(0, W), pl.ds(W, W)
        far_r = pl.ds(2 * rows + r0, RB)
        moves = ((h_st.at[sl, :, left], h_out.at[r, frow(cx, c)]), (h_st.at[sl, :, right], h_out.at[r, frow(1 - cx, c)]),
                 (dc_st.at[sl, :, left], dc_out.at[r, mine(c)]))
        pushes = ((h_st.at[sl, :, left], h_out.at[far_r, frow(cx, c)]), (h_st.at[sl, :, right], h_out.at[far_r, frow(1 - cx, c)]),
                  (dc_st.at[sl, :, right], dc_out.at[far_r, mine(c)]))
        return ([pltpu.make_async_copy(src, dst, out_sem.at[sl, i]) for i, (src, dst) in enumerate(moves)],
                [remote(src, dst, push_send.at[sl, i], push_recv.at[n, i], to_d) for i, (src, dst) in enumerate(pushes)])

    def extra(n, c):
        sl = lax.rem(n, 2)
        cols = pl.ds(pl.multiple_of((c - split) * W, W), W)
        return [pltpu.make_async_copy(dc_st.at[sl, :, pl.ds(0, W)], dcp_own.at[:, cols], extra_sem.at[0]),
                pltpu.make_async_copy(dc_st.at[sl, :, pl.ds(W, W)], dcp_oth.at[:, cols], extra_sem.at[1])]

    steps = 2 * chunks

    def drain(first, last):
        @pl.loop(first, last)
        def _(c):
            for copy in over_x(c) + over_d(c):
                copy.wait_send()

    @pl.loop(0, steps)
    def _(s):
        paired = s >= 2 * split
        c = jnp.where(paired, s // 2, jnp.where(s < SLOTS, s, jnp.where(s < SLOTS + split, s - SLOTS, s - split)))
        half = jnp.where(paired, lax.rem(s, 2), jnp.where((s >= SLOTS) & (s < SLOTS + split), 1, 0))
        odd = lax.rem(s, 2) == 1
        single = (s >= 2 * SLOTS - 1) & (s < SLOTS + split - 1)
        ahead = single | ((s >= 2 * split - 1) & odd & (s < steps - 1))
        hc = jnp.where(single, s - SLOTS + 1, (s + 1) // 2)

        def arrive(c):
            for copy in over_x(c):
                copy.wait_recv()
            for copy in over_d(c):
                copy.start()

            @pl.when(c + AHEAD < chunks)
            def _():
                for copy in over_x(c + AHEAD):
                    copy.start()

            for copy in loads(c, False):
                copy.start()

        def arrive_late(c):
            for copy in over_d(c):
                copy.wait_recv()
            for copy in loads(c, True):
                copy.start()

        @pl.when(s < SLOTS)
        def _():
            arrive(s)
            arrive_late(s)

        @pl.when((s < SLOTS) | ((s >= 2 * SLOTS) & (s < SLOTS + split)) | (paired & ~odd))
        def _():
            for copy in loads(c, False) + loads(c, True):
                copy.wait()

        @pl.when(s == SLOTS + split)
        def _():
            part_save.start()
            up_tail.wait_recv()
            up_tail_d.start()
            part_save.wait()
            part_send.start()

        @pl.when(ahead)
        def _():
            arrive(hc)

        @pl.when(s == SLOTS)
        def _():
            x2.wait_recv()
            z2.wait_recv()
            for copy in saves + shares:
                copy.start()
            x3.wait_recv()
            z3.wait_recv()

        @pl.when(s == steps - 4)
        def _():
            for copy in saves:
                copy.wait()
            for copy in shares:
                copy.wait_send()
                copy.wait_recv()
            up_tail_d.wait_recv()
            for copy in (x1, z1, x2, z2, x3, z3, up_all, down_all, up_tail, up_tail_d):
                copy.wait_send()
            drain(0, chunks - 4)

        @pl.when(s == steps - 1)
        def _():
            own_save.start()

        slot = lax.rem(c, SLOTS)
        r0 = pl.multiple_of(half * rows, RB)
        sl = lax.rem(s, 2)
        cc = jnp.dot(xv[pl.ds(r0, RB), :], uv[slot], preferred_element_type=F32)
        dh = lax.dot_general(zv[pl.ds(r0, RB), :], vv[slot], LAST, preferred_element_type=F32)
        h, slope = gelu_parts(cc.astype(BF16).astype(F32))
        dc = (dh * slope).astype(BF16)

        @pl.when(s >= 2)
        def _():
            keep, push = outs(s - 2, c, r0)
            for copy in keep:
                copy.wait()
            for copy in push:
                copy.wait_send()
                copy.wait_recv()

        @pl.when((s >= 2 * split + 3) & odd)
        def _():
            for copy in extra(s, c):
                copy.wait()

        h_st[sl] = h.astype(BF16)
        dc_st[sl] = dc

        @pl.when(ahead)
        def _():
            arrive_late(hc)

        @pl.when((half == 0) | (c < split))
        def _():
            acc[pl.ds(r0, RB), :] += lax.dot_general(dc_st[sl], uv[slot, near, :], LAST, preferred_element_type=F32)

        keep, push = outs(s, c, r0)
        for copy in keep + push:
            copy.start()

        @pl.when((half == 1) & (c >= split))
        def _():
            for copy in extra(s, c):
                copy.start()

    for n in range(2):
        keep, push = outs(steps - 2 + n, 0, 0)
        for copy in keep:
            copy.wait()
        for copy in push:
            copy.wait_send()
            copy.wait_recv()
    for copy in extra(1, split):
        copy.wait()
    own_save.wait()
    part_send.wait_recv()
    part_send.wait_send()
    drain(chunks - 4, chunks)


def hidden_call(x_act, w_up, w_down, z_grad):
    rows, dk = x_act.shape
    ffc = w_up.shape[1]
    ff, dq = w_down.shape
    chunks = ffc // W
    flops = 2 * rows * 2 * ff * dk * 5
    hbm = pl.BlockSpec(memory_space=pl.ANY)
    sds = jax.ShapeDtypeStruct
    out_shape = [
        sds((4 * rows, ff), BF16), sds((4 * rows, ffc), BF16), sds((4 * rows, dk), BF16), sds((4 * rows, dq), BF16),
        sds((rows, dk), F32), sds((rows, dk), F32), sds((rows, dk), F32),
        sds((rows, PHI * W), BF16), sds((rows, PHI * W), BF16), sds((dk, PHI * W), BF16), sds((dk, PHI * W), BF16),
        sds(w_up.shape, BF16), sds(w_up.shape, BF16), sds(w_up.shape, BF16),
        sds(w_down.shape, BF16), sds(w_down.shape, BF16), sds(w_down.shape, BF16),
    ]
    dma = pltpu.SemaphoreType.DMA
    return pl.pallas_call(
        hidden_kernel,
        in_specs=[hbm] * 4,
        out_specs=[hbm] * len(out_shape),
        out_shape=out_shape,
        scratch_shapes=[
            pltpu.VMEM((2 * rows, 2 * dk), BF16), pltpu.VMEM((2 * rows, 2 * dk), BF16),
            pltpu.VMEM((SLOTS, 2 * dk, 2 * W), BF16), pltpu.VMEM((SLOTS, 2 * W, 2 * dk), BF16),
            pltpu.VMEM((2 * rows, dk), F32),
            pltpu.VMEM((2, RB, 2 * W), BF16), pltpu.VMEM((2, RB, 2 * W), BF16),
            dma((6,)), dma((6,)), dma((chunks, 3)), dma((chunks, 3)), dma((chunks, 3)), dma((chunks, 3)),
            dma((7,)), dma((7,)), dma((12,)), dma((5,)), dma((2, 3)), dma((2,)), dma((2, 3)), dma((4 * ffc // (2 * W), 3)),
        ],
        compiler_params=pltpu.CompilerParams(
            collective_id=0, has_side_effects=True, vmem_limit_bytes=67_000_000),
        cost_estimate=pl.CostEstimate(flops=flops, bytes_accessed=200_000_000, transcendentals=2 * rows * ff),
        name="hidden",
    )(x_act, w_up, w_down, z_grad)


def solution(mesh):
    row_spec = P(("dp", "cx", "cz"), "cy")
    up_spec = P("cy", ("cz", "cx"))
    down_spec = P("cz", ("cy", "cx"))
    up_out = P(("dp", "cy"), ("cz", "cx"))
    down_out = P(("dp", "cz"), ("cy", "cx"))
    swap = [(0, 1), (1, 0)]

    def local_step(x_act, w_up, w_down, z_grad):
        h, dc, xs, zs, dx_own, _, dx_got, dcp_own, dcp_oth, up_y, up_yd = hidden_call(x_act, w_up, w_down, z_grad)[:11]
        dcr_own = lax.ppermute(dcp_own, "cz", swap)
        dcr_oth = lax.ppermute(dcp_oth, "cz", swap)
        down_grad = lax.dot_general(h, zs, FIRST, preferred_element_type=F32).astype(BF16)
        up_grad = lax.dot_general(xs, dc, FIRST, preferred_element_type=F32).astype(BF16)
        dx = lax.dot_general(dcr_own, up_y, LAST, preferred_element_type=F32) + (dx_own + dx_got)
        x_grad = (lax.dot_general(dcr_oth, up_yd, LAST, preferred_element_type=F32) + dx).astype(BF16)
        return (x_grad, up_grad, down_grad)

    return jax.shard_map(local_step, mesh=mesh, in_specs=(row_spec, up_spec, down_spec, row_spec), out_specs=(row_spec, up_out, down_out), check_vma=False)
```

```python
import math
import jax
import jax.numpy as jnp
from jax import lax
from jax.experimental import pallas as pl
from jax.experimental.pallas import tpu as pltpu
from jax.sharding import PartitionSpec as P

GELU_COEF = 0.044715
SQRT_TWO_PI = math.sqrt(2.0 / math.pi)
LAST = (((1,), (1,)), ((), ()))
FIRST = (((0,), (0,)), ((), ()))
F32 = jnp.float32
BF16 = jnp.bfloat16
MESH = pl.DeviceIdType.MESH


W = 128
RB = 1024
PHI = 8
AHEAD = 8
SLOTS = 8


def gelu_parts(c):
    c2 = c * c
    t = jnp.tanh(SQRT_TWO_PI * (c * (1.0 + GELU_COEF * c2)))
    half = 0.5 * (1.0 + t)
    slope = half + 0.5 * c * (1.0 - t * t) * SQRT_TWO_PI * (1.0 + 3.0 * GELU_COEF * c2)
    return c * half, slope


def hidden_kernel(x_in, up, down, z_in,
                  h_out, dc_out, x_out, z_out, dx_own, dx_part, dx_got, dc_first, dc_got, dcp_own, dcp_oth, up_y0, up_y, up_yd, up_d, up_x, up_xd, down_d, down_x, down_xd,
                  xv, zv, uv, vv, acc, h_st, dc_st,
                  act_send, act_recv, wx_send, wx_recv, wd_send, wd_recv, all_send, all_recv,
                  load_sem, local_sem, out_sem, extra_sem, push_send, push_recv):
    cz, cy, cx = lax.axis_index("cz"), lax.axis_index("cy"), lax.axis_index("cx")
    to_x, to_y, to_d = {"cy": 1 - cy}, {"cz": 1 - cz}, {"cx": 1 - cx}
    rows, dk = x_in.shape
    ffc = up.shape[1]
    dq = down.shape[1]
    chunks = ffc // W

    def remote(src, dst, send, recv, dev):
        return pltpu.make_async_remote_copy(src_ref=src, dst_ref=dst, send_sem=send, recv_sem=recv,
                                            device_id=dev, device_id_type=MESH)

    def mine(c):
        return pl.ds(pl.multiple_of(c * W, W), W)

    def frow(f, c):
        return pl.ds(pl.multiple_of(f * ffc + c * W, W), W)

    own, oth = pl.ds(0, rows), pl.ds(rows, rows)
    near, far = pl.ds(0, dk), pl.ds(dk, dk)

    x1 = remote(x_in, xv.at[own, far], act_send.at[0], act_recv.at[0], to_x)
    z1 = remote(z_in, zv.at[own, far], act_send.at[1], act_recv.at[1], to_x)
    x2 = remote(x_in, xv.at[oth, near], act_send.at[2], act_recv.at[2], to_y)
    z2 = remote(z_in, zv.at[oth, near], act_send.at[3], act_recv.at[3], to_y)
    x3 = remote(xv.at[own, far], xv.at[oth, far], act_send.at[4], act_recv.at[4], to_y)
    z3 = remote(zv.at[own, far], zv.at[oth, far], act_send.at[5], act_recv.at[5], to_y)
    up_all = remote(up, up_d, all_send.at[0], all_recv.at[0], to_d)
    down_all = remote(down, down_d, all_send.at[1], all_recv.at[1], to_d)

    split = chunks - PHI
    head, tail = pl.ds(split * W, W), pl.ds((split + 1) * W, (PHI - 1) * W)
    up_tail = [remote(up.at[:, head], up_y0, all_send.at[2], all_recv.at[2], to_y),
               remote(up.at[:, tail], up_y, all_send.at[7], all_recv.at[7], to_y)]
    up_tail_d = [remote(up_y0, up_yd.at[:, pl.ds(0, W)], all_send.at[3], all_recv.at[3], to_d),
                 remote(up_y, up_yd.at[:, pl.ds(W, (PHI - 1) * W)], all_send.at[8], all_recv.at[8], to_d)]
    first_send = remote(dc_first, dc_got, all_send.at[9], all_recv.at[9], to_y)
    part_save = pltpu.make_async_copy(acc.at[oth], dx_part, local_sem.at[3])
    part_send = remote(dx_part, dx_got, all_send.at[4], all_recv.at[4], to_y)
    own_save = pltpu.make_async_copy(acc.at[own], dx_own, local_sem.at[4])

    def over_x(c):
        return [remote(up.at[:, mine(c)], up_x.at[:, mine(c)], wx_send.at[c, 0], wx_recv.at[c, 0], to_x)] + [
            remote(down.at[frow(f, c)], down_x.at[frow(f, c)], wx_send.at[c, 1 + f], wx_recv.at[c, 1 + f], to_x)
            for f in range(2)]

    def over_d(c):
        return [remote(up_x.at[:, mine(c)], up_xd.at[:, mine(c)], wd_send.at[c, 0], wd_recv.at[c, 0], to_d)] + [
            remote(down_x.at[frow(f, c)], down_xd.at[frow(f, c)], wd_send.at[c, 1 + f], wd_recv.at[c, 1 + f], to_d)
            for f in range(2)]

    def lanes(part, core):
        return pl.ds(pl.multiple_of(part * dk + core * dq, 128), dq)

    def loads(c, late):
        slot = lax.rem(c, SLOTS)
        left, right = pl.ds(0, W), pl.ds(W, W)
        if late:
            moves = [(up_xd.at[:, mine(c)], uv.at[slot, far, right])]
            parts = [(down_xd, lanes(1, 1 - cx))]
        else:
            moves = [(up.at[:, mine(c)], uv.at[slot, near, left]),
                     (up_d.at[:, mine(c)], uv.at[slot, near, right]),
                     (up_x.at[:, mine(c)], uv.at[slot, far, left])]
            parts = [(down, lanes(0, cx)), (down_d, lanes(0, 1 - cx)), (down_x, lanes(1, cx))]
        for src, lane in parts:
            moves.append((src.at[frow(cx, c)], vv.at[slot, left, lane]))
            moves.append((src.at[frow(1 - cx, c)], vv.at[slot, right, lane]))
        base = 9 if late else 0
        return [pltpu.make_async_copy(s, d, load_sem.at[base + i]) for i, (s, d) in enumerate(moves)]

    barrier = pltpu.get_barrier_semaphore()
    for dev in (to_x, to_y, to_d):
        pl.semaphore_signal(barrier, inc=1, device_id=dev, device_id_type=MESH)
    pl.semaphore_wait(barrier, 3)

    x1.start()
    x2.start()
    z1.start()
    z2.start()
    for c in range(AHEAD):
        for copy in over_x(c):
            copy.start()
    up_all.start()
    down_all.start()
    x0 = pltpu.make_async_copy(x_in, xv.at[own, near], local_sem.at[0])
    z0 = pltpu.make_async_copy(z_in, zv.at[own, near], local_sem.at[1])
    x0.start()
    z0.start()

    @pl.loop(0, 2 * rows // 256)
    def _(i):
        acc[pl.ds(pl.multiple_of(i * 256, 256), 256), :] = jnp.zeros((256, dk), F32)

    x1.wait_recv()
    x3.start()
    z1.wait_recv()
    z3.start()
    for copy in up_tail:
        copy.start()
    x0.wait()
    z0.wait()
    up_all.wait_recv()
    down_all.wait_recv()
    mine_all, core_all = pl.ds(0, 2 * rows), pl.ds(2 * rows, 2 * rows)
    saves = [pltpu.make_async_copy(xv.at[:, near], x_out.at[mine_all], local_sem.at[0]),
             pltpu.make_async_copy(zv.at[:, lanes(0, cx)], z_out.at[mine_all], local_sem.at[1])]
    shares = [remote(xv.at[:, near], x_out.at[core_all], all_send.at[5], all_recv.at[5], to_d),
              remote(zv.at[:, lanes(0, 1 - cx)], z_out.at[core_all], all_send.at[6], all_recv.at[6], to_d)]

    def outs(n, c, r0):
        sl = lax.rem(n, 2)
        r = pl.ds(r0, RB)
        left, right = pl.ds(0, W), pl.ds(W, W)
        far_r = pl.ds(2 * rows + r0, RB)
        moves = ((h_st.at[sl, :, left], h_out.at[r, frow(cx, c)]), (h_st.at[sl, :, right], h_out.at[r, frow(1 - cx, c)]),
                 (dc_st.at[sl, :, left], dc_out.at[r, mine(c)]))
        pushes = ((h_st.at[sl, :, left], h_out.at[far_r, frow(cx, c)]), (h_st.at[sl, :, right], h_out.at[far_r, frow(1 - cx, c)]),
                  (dc_st.at[sl, :, right], dc_out.at[far_r, mine(c)]))
        return ([pltpu.make_async_copy(src, dst, out_sem.at[sl, i]) for i, (src, dst) in enumerate(moves)],
                [remote(src, dst, push_send.at[sl, i], push_recv.at[n, i], to_d) for i, (src, dst) in enumerate(pushes)])

    def extra(n, c, first):
        sl = lax.rem(n, 2)
        base = pl.ds(pl.multiple_of((c - split) * W, W), W)
        own_dst = dc_first if first else dcp_own.at[:, pl.ds(pl.multiple_of((c - split - 1) * W, W), W)]
        return [pltpu.make_async_copy(dc_st.at[sl, :, pl.ds(0, W)], own_dst, extra_sem.at[0]),
                pltpu.make_async_copy(dc_st.at[sl, :, pl.ds(W, W)], dcp_oth.at[:, base], extra_sem.at[1])]

    steps = 2 * chunks

    def drain(first, last):
        @pl.loop(first, last)
        def _(c):
            for copy in over_x(c) + over_d(c):
                copy.wait_send()

    @pl.loop(0, steps)
    def _(s):
        paired = s >= 2 * split
        c = jnp.where(paired, s // 2, jnp.where(s < SLOTS, s, jnp.where(s < SLOTS + split, s - SLOTS, s - split)))
        half = jnp.where(paired, lax.rem(s, 2), jnp.where((s >= SLOTS) & (s < SLOTS + split), 1, 0))
        odd = lax.rem(s, 2) == 1
        single = (s >= 2 * SLOTS - 1) & (s < SLOTS + split - 1)
        ahead = single | ((s >= 2 * split - 1) & odd & (s < steps - 1))
        hc = jnp.where(single, s - SLOTS + 1, (s + 1) // 2)

        def arrive(c):
            for copy in over_x(c):
                copy.wait_recv()
            for copy in over_d(c):
                copy.start()

            @pl.when(c + AHEAD < chunks)
            def _():
                for copy in over_x(c + AHEAD):
                    copy.start()

            for copy in loads(c, False):
                copy.start()

        def arrive_late(c):
            for copy in over_d(c):
                copy.wait_recv()
            for copy in loads(c, True):
                copy.start()

        @pl.when(s < SLOTS)
        def _():
            arrive(s)
            arrive_late(s)

        @pl.when((s < SLOTS) | ((s >= 2 * SLOTS) & (s < SLOTS + split)) | (paired & ~odd))
        def _():
            for copy in loads(c, False) + loads(c, True):
                copy.wait()

        @pl.when(s == SLOTS + split)
        def _():
            part_save.start()
            for copy, onward in zip(up_tail, up_tail_d):
                copy.wait_recv()
                onward.start()
            part_save.wait()
            part_send.start()

        @pl.when(ahead)
        def _():
            arrive(hc)

        @pl.when(s == SLOTS)
        def _():
            x2.wait_recv()
            z2.wait_recv()
            for copy in saves + shares:
                copy.start()
            x3.wait_recv()
            z3.wait_recv()

        @pl.when(s == steps - 4)
        def _():
            for copy in saves:
                copy.wait()
            for copy in shares:
                copy.wait_send()
                copy.wait_recv()
            for copy in up_tail_d:
                copy.wait_recv()
            for copy in [x1, z1, x2, z2, x3, z3, up_all, down_all] + up_tail + up_tail_d:
                copy.wait_send()
            drain(0, chunks - 4)

        @pl.when(s == steps - 1)
        def _():
            own_save.start()

        slot = lax.rem(c, SLOTS)
        r0 = pl.multiple_of(half * rows, RB)
        sl = lax.rem(s, 2)
        cc = jnp.dot(xv[pl.ds(r0, RB), :], uv[slot], preferred_element_type=F32)
        dh = lax.dot_general(zv[pl.ds(r0, RB), :], vv[slot], LAST, preferred_element_type=F32)
        h, slope = gelu_parts(cc.astype(BF16).astype(F32))
        dc = (dh * slope).astype(BF16)

        @pl.when(s >= 2)
        def _():
            keep, push = outs(s - 2, c, r0)
            for copy in keep:
                copy.wait()
            for copy in push:
                copy.wait_send()
                copy.wait_recv()

        @pl.when((s >= 2 * split + 3) & odd)
        def _():
            for copy in extra(s, c, True):
                copy.wait()

        @pl.when(s == 2 * split + 3)
        def _():
            first_send.start()

        h_st[sl] = h.astype(BF16)
        dc_st[sl] = dc

        @pl.when(ahead)
        def _():
            arrive_late(hc)

        @pl.when((half == 0) | (c < split))
        def _():
            acc[pl.ds(r0, RB), :] += lax.dot_general(dc_st[sl], uv[slot, near, :], LAST, preferred_element_type=F32)

        keep, push = outs(s, c, r0)
        for copy in keep + push:
            copy.start()

        @pl.when((half == 1) & (c == split))
        def _():
            for copy in extra(s, c, True):
                copy.start()

        @pl.when((half == 1) & (c > split))
        def _():
            for copy in extra(s, c, False):
                copy.start()

    for n in range(2):
        keep, push = outs(steps - 2 + n, 0, 0)
        for copy in keep:
            copy.wait()
        for copy in push:
            copy.wait_send()
            copy.wait_recv()
    for copy in extra(1, split, True):
        copy.wait()
    own_save.wait()
    part_send.wait_recv()
    part_send.wait_send()
    first_send.wait_recv()
    first_send.wait_send()
    drain(chunks - 4, chunks)


def hidden_call(x_act, w_up, w_down, z_grad):
    rows, dk = x_act.shape
    ffc = w_up.shape[1]
    ff, dq = w_down.shape
    chunks = ffc // W
    flops = 2 * rows * 2 * ff * dk * 5
    hbm = pl.BlockSpec(memory_space=pl.ANY)
    sds = jax.ShapeDtypeStruct
    out_shape = [
        sds((4 * rows, ff), BF16), sds((4 * rows, ffc), BF16), sds((4 * rows, dk), BF16), sds((4 * rows, dq), BF16),
        sds((rows, dk), F32), sds((rows, dk), F32), sds((rows, dk), F32),
        sds((rows, W), BF16), sds((rows, W), BF16), sds((rows, (PHI - 1) * W), BF16), sds((rows, PHI * W), BF16),
        sds((dk, W), BF16), sds((dk, (PHI - 1) * W), BF16), sds((dk, PHI * W), BF16),
        sds(w_up.shape, BF16), sds(w_up.shape, BF16), sds(w_up.shape, BF16),
        sds(w_down.shape, BF16), sds(w_down.shape, BF16), sds(w_down.shape, BF16),
    ]
    dma = pltpu.SemaphoreType.DMA
    return pl.pallas_call(
        hidden_kernel,
        in_specs=[hbm] * 4,
        out_specs=[hbm] * len(out_shape),
        out_shape=out_shape,
        scratch_shapes=[
            pltpu.VMEM((2 * rows, 2 * dk), BF16), pltpu.VMEM((2 * rows, 2 * dk), BF16),
            pltpu.VMEM((SLOTS, 2 * dk, 2 * W), BF16), pltpu.VMEM((SLOTS, 2 * W, 2 * dk), BF16),
            pltpu.VMEM((2 * rows, dk), F32),
            pltpu.VMEM((2, RB, 2 * W), BF16), pltpu.VMEM((2, RB, 2 * W), BF16),
            dma((6,)), dma((6,)), dma((chunks, 3)), dma((chunks, 3)), dma((chunks, 3)), dma((chunks, 3)),
            dma((10,)), dma((10,)), dma((12,)), dma((5,)), dma((2, 3)), dma((2,)), dma((2, 3)), dma((4 * ffc // (2 * W), 3)),
        ],
        compiler_params=pltpu.CompilerParams(
            collective_id=0, has_side_effects=True, vmem_limit_bytes=67_000_000),
        cost_estimate=pl.CostEstimate(flops=flops, bytes_accessed=200_000_000, transcendentals=2 * rows * ff),
        name="hidden",
    )(x_act, w_up, w_down, z_grad)


def solution(mesh):
    row_spec = P(("dp", "cx", "cz"), "cy")
    up_spec = P("cy", ("cz", "cx"))
    down_spec = P("cz", ("cy", "cx"))
    up_out = P(("dp", "cy"), ("cz", "cx"))
    down_out = P(("dp", "cz"), ("cy", "cx"))
    swap = [(0, 1), (1, 0)]

    def local_step(x_act, w_up, w_down, z_grad):
        (h, dc, xs, zs, dx_own, _, dx_got, _, dc_got, dcp_own, dcp_oth, up_y0, up_y, up_yd) = hidden_call(
            x_act, w_up, w_down, z_grad)[:14]
        dcr_own = lax.ppermute(dcp_own, "cz", swap)
        dcr_oth = lax.ppermute(dcp_oth, "cz", swap)
        down_grad = lax.dot_general(h, zs, FIRST, preferred_element_type=F32).astype(BF16)
        up_grad = lax.dot_general(xs, dc, FIRST, preferred_element_type=F32).astype(BF16)
        dx = lax.dot_general(dc_got, up_y0, LAST, preferred_element_type=F32) + (dx_own + dx_got)
        dx = lax.dot_general(dcr_own, up_y, LAST, preferred_element_type=F32) + dx
        x_grad = (lax.dot_general(dcr_oth, up_yd, LAST, preferred_element_type=F32) + dx).astype(BF16)
        return (x_grad, up_grad, down_grad)

    return jax.shard_map(local_step, mesh=mesh, in_specs=(row_spec, up_spec, down_spec, row_spec), out_specs=(row_spec, up_out, down_out), check_vma=False)
```

```python
import math
import jax
import jax.numpy as jnp
from jax import lax
from jax.experimental import pallas as pl
from jax.experimental.pallas import tpu as pltpu
from jax.sharding import PartitionSpec as P

GELU_COEF = 0.044715
SQRT_TWO_PI = math.sqrt(2.0 / math.pi)
LAST = (((1,), (1,)), ((), ()))
FIRST = (((0,), (0,)), ((), ()))
F32 = jnp.float32
BF16 = jnp.bfloat16
MESH = pl.DeviceIdType.MESH


W = 128
RB = 1024
PHI = 8
AHEAD = 8
SLOTS = 8


def gelu_parts(c):
    c2 = c * c
    t = jnp.tanh(SQRT_TWO_PI * (c * (1.0 + GELU_COEF * c2)))
    half = 0.5 * (1.0 + t)
    slope = half + 0.5 * c * (1.0 - t * t) * SQRT_TWO_PI * (1.0 + 3.0 * GELU_COEF * c2)
    return c * half, slope


def hidden_kernel(x_in, up, down, z_in,
                  h_out, dc_out, x_out, z_out, dx_own, dx_part, dx_got, dc_first, dc_got, dcp_own, dcp_oth, up_y0, up_y, up_yd, up_d, up_x, up_xd, down_d, down_x, down_xd,
                  xv, zv, uv, vv, acc, h_st, dc_st,
                  act_send, act_recv, wx_send, wx_recv, wd_send, wd_recv, all_send, all_recv,
                  load_sem, local_sem, out_sem, extra_sem, push_send, push_recv):
    cz, cy, cx = lax.axis_index("cz"), lax.axis_index("cy"), lax.axis_index("cx")
    to_x, to_y, to_d = {"cy": 1 - cy}, {"cz": 1 - cz}, {"cx": 1 - cx}
    rows, dk = x_in.shape
    ffc = up.shape[1]
    dq = down.shape[1]
    chunks = ffc // W

    def remote(src, dst, send, recv, dev):
        return pltpu.make_async_remote_copy(src_ref=src, dst_ref=dst, send_sem=send, recv_sem=recv,
                                            device_id=dev, device_id_type=MESH)

    def mine(c):
        return pl.ds(pl.multiple_of(c * W, W), W)

    def frow(f, c):
        return pl.ds(pl.multiple_of(f * ffc + c * W, W), W)

    own, oth = pl.ds(0, rows), pl.ds(rows, rows)
    near, far = pl.ds(0, dk), pl.ds(dk, dk)

    x1 = remote(x_in, xv.at[own, far], act_send.at[0], act_recv.at[0], to_x)
    z1 = remote(z_in, zv.at[own, far], act_send.at[1], act_recv.at[1], to_x)
    x2 = remote(x_in, xv.at[oth, near], act_send.at[2], act_recv.at[2], to_y)
    z2 = remote(z_in, zv.at[oth, near], act_send.at[3], act_recv.at[3], to_y)
    x3 = remote(xv.at[own, far], xv.at[oth, far], act_send.at[4], act_recv.at[4], to_y)
    z3 = remote(zv.at[own, far], zv.at[oth, far], act_send.at[5], act_recv.at[5], to_y)
    up_all = remote(up, up_d, all_send.at[0], all_recv.at[0], to_d)
    down_all = remote(down, down_d, all_send.at[1], all_recv.at[1], to_d)

    split = chunks - PHI
    head, tail = pl.ds(split * W, W), pl.ds((split + 1) * W, (PHI - 1) * W)
    up_tail = [remote(up.at[:, head], up_y0, all_send.at[2], all_recv.at[2], to_y),
               remote(up.at[:, tail], up_y, all_send.at[7], all_recv.at[7], to_y)]
    up_tail_d = [remote(up_y0, up_yd.at[:, pl.ds(0, W)], all_send.at[3], all_recv.at[3], to_d),
                 remote(up_y, up_yd.at[:, pl.ds(W, (PHI - 1) * W)], all_send.at[8], all_recv.at[8], to_d)]
    first_send = remote(dc_first, dc_got, all_send.at[9], all_recv.at[9], to_y)
    part_save = pltpu.make_async_copy(acc.at[oth], dx_part, local_sem.at[3])
    part_send = remote(dx_part, dx_got, all_send.at[4], all_recv.at[4], to_y)
    own_save = pltpu.make_async_copy(acc.at[own], dx_own, local_sem.at[4])

    def over_x(c):
        return [remote(up.at[:, mine(c)], up_x.at[:, mine(c)], wx_send.at[c, 0], wx_recv.at[c, 0], to_x)] + [
            remote(down.at[frow(f, c)], down_x.at[frow(f, c)], wx_send.at[c, 1 + f], wx_recv.at[c, 1 + f], to_x)
            for f in range(2)]

    def over_d(c):
        return [remote(up_x.at[:, mine(c)], up_xd.at[:, mine(c)], wd_send.at[c, 0], wd_recv.at[c, 0], to_d)] + [
            remote(down_x.at[frow(f, c)], down_xd.at[frow(f, c)], wd_send.at[c, 1 + f], wd_recv.at[c, 1 + f], to_d)
            for f in range(2)]

    def lanes(part, core):
        return pl.ds(pl.multiple_of(part * dk + core * dq, 128), dq)

    def loads(c, late):
        slot = lax.rem(c, SLOTS)
        left, right = pl.ds(0, W), pl.ds(W, W)
        if late:
            moves = [(up_xd.at[:, mine(c)], uv.at[slot, far, right])]
            parts = [(down_xd, lanes(1, 1 - cx))]
        else:
            moves = [(up.at[:, mine(c)], uv.at[slot, near, left]),
                     (up_d.at[:, mine(c)], uv.at[slot, near, right]),
                     (up_x.at[:, mine(c)], uv.at[slot, far, left])]
            parts = [(down, lanes(0, cx)), (down_d, lanes(0, 1 - cx)), (down_x, lanes(1, cx))]
        for src, lane in parts:
            moves.append((src.at[frow(cx, c)], vv.at[slot, left, lane]))
            moves.append((src.at[frow(1 - cx, c)], vv.at[slot, right, lane]))
        base = 9 if late else 0
        return [pltpu.make_async_copy(s, d, load_sem.at[base + i]) for i, (s, d) in enumerate(moves)]

    barrier = pltpu.get_barrier_semaphore()
    for dev in (to_x, to_y, to_d):
        pl.semaphore_signal(barrier, inc=1, device_id=dev, device_id_type=MESH)
    pl.semaphore_wait(barrier, 3)

    x1.start()
    x2.start()
    z1.start()
    z2.start()
    for c in range(AHEAD):
        for copy in over_x(c):
            copy.start()
    up_all.start()
    down_all.start()
    x0 = pltpu.make_async_copy(x_in, xv.at[own, near], local_sem.at[0])
    z0 = pltpu.make_async_copy(z_in, zv.at[own, near], local_sem.at[1])
    x0.start()
    z0.start()

    @pl.loop(0, 2 * rows // 256)
    def _(i):
        acc[pl.ds(pl.multiple_of(i * 256, 256), 256), :] = jnp.zeros((256, dk), F32)

    x1.wait_recv()
    x3.start()
    z1.wait_recv()
    z3.start()
    for copy in up_tail:
        copy.start()
    x0.wait()
    z0.wait()
    up_all.wait_recv()
    down_all.wait_recv()
    mine_all, core_all = pl.ds(0, 2 * rows), pl.ds(2 * rows, 2 * rows)
    saves = [pltpu.make_async_copy(xv.at[:, near], x_out.at[mine_all], local_sem.at[0]),
             pltpu.make_async_copy(zv.at[:, lanes(0, cx)], z_out.at[mine_all], local_sem.at[1])]
    shares = [remote(xv.at[:, near], x_out.at[core_all], all_send.at[5], all_recv.at[5], to_d),
              remote(zv.at[:, lanes(0, 1 - cx)], z_out.at[core_all], all_send.at[6], all_recv.at[6], to_d)]

    def outs(n, c, r0):
        sl = lax.rem(n, 2)
        r = pl.ds(r0, RB)
        left, right = pl.ds(0, W), pl.ds(W, W)
        far_r = pl.ds(2 * rows + r0, RB)
        moves = ((h_st.at[sl, :, left], h_out.at[r, frow(cx, c)]), (h_st.at[sl, :, right], h_out.at[r, frow(1 - cx, c)]),
                 (dc_st.at[sl, :, left], dc_out.at[r, mine(c)]))
        pushes = ((h_st.at[sl, :, left], h_out.at[far_r, frow(cx, c)]), (h_st.at[sl, :, right], h_out.at[far_r, frow(1 - cx, c)]),
                  (dc_st.at[sl, :, right], dc_out.at[far_r, mine(c)]))
        return ([pltpu.make_async_copy(src, dst, out_sem.at[sl, i]) for i, (src, dst) in enumerate(moves)],
                [remote(src, dst, push_send.at[sl, i], push_recv.at[n, i], to_d) for i, (src, dst) in enumerate(pushes)])

    def extra(n, c, first):
        sl = lax.rem(n, 2)
        base = pl.ds(pl.multiple_of((c - split) * W, W), W)
        own_dst = dc_first if first else dcp_own.at[:, pl.ds(pl.multiple_of((c - split - 1) * W, W), W)]
        return [pltpu.make_async_copy(dc_st.at[sl, :, pl.ds(0, W)], own_dst, extra_sem.at[0]),
                pltpu.make_async_copy(dc_st.at[sl, :, pl.ds(W, W)], dcp_oth.at[:, base], extra_sem.at[1])]

    steps = 2 * chunks

    def drain(first, last):
        @pl.loop(first, last)
        def _(c):
            for copy in over_x(c) + over_d(c):
                copy.wait_send()

    @pl.loop(0, steps)
    def _(s):
        paired = s >= 2 * split
        c = jnp.where(paired, s // 2, jnp.where(s < SLOTS, s, jnp.where(s < SLOTS + split, s - SLOTS, s - split)))
        half = jnp.where(paired, lax.rem(s, 2), jnp.where((s >= SLOTS) & (s < SLOTS + split), 1, 0))
        odd = lax.rem(s, 2) == 1
        single = (s >= 2 * SLOTS - 1) & (s < SLOTS + split - 1)
        ahead = single | ((s >= 2 * split - 1) & odd & (s < steps - 1))
        hc = jnp.where(single, s - SLOTS + 1, (s + 1) // 2)

        def arrive(c):
            for copy in over_x(c):
                copy.wait_recv()
            for copy in over_d(c):
                copy.start()

            @pl.when(c + AHEAD < chunks)
            def _():
                for copy in over_x(c + AHEAD):
                    copy.start()

            for copy in loads(c, False):
                copy.start()

        def arrive_late(c):
            for copy in over_d(c):
                copy.wait_recv()
            for copy in loads(c, True):
                copy.start()

        @pl.when(s < SLOTS)
        def _():
            arrive(s)
            arrive_late(s)

        @pl.when((s < SLOTS) | ((s >= 2 * SLOTS) & (s < SLOTS + split)) | (paired & ~odd))
        def _():
            for copy in loads(c, False) + loads(c, True):
                copy.wait()

        @pl.when(s == SLOTS + split)
        def _():
            part_save.start()
            for copy, onward in zip(up_tail, up_tail_d):
                copy.wait_recv()
                onward.start()
            part_save.wait()
            part_send.start()

        @pl.when(ahead)
        def _():
            arrive(hc)

        @pl.when(s == SLOTS)
        def _():
            x2.wait_recv()
            z2.wait_recv()
            for copy in saves + shares:
                copy.start()
            x3.wait_recv()
            z3.wait_recv()

        @pl.when(s == steps - 4)
        def _():
            for copy in saves:
                copy.wait()
            for copy in shares:
                copy.wait_send()
                copy.wait_recv()
            for copy in up_tail_d:
                copy.wait_recv()
            for copy in [x1, z1, x2, z2, x3, z3, up_all, down_all] + up_tail + up_tail_d:
                copy.wait_send()
            drain(0, chunks - 4)

        @pl.when(s == steps - 1)
        def _():
            own_save.start()

        slot = lax.rem(c, SLOTS)
        r0 = pl.multiple_of(half * rows, RB)
        sl = lax.rem(s, 2)

        @pl.when(s >= 2)
        def _():
            keep, push = outs(s - 2, c, r0)
            for copy in keep:
                copy.wait()
            for copy in push:
                copy.wait_send()
                copy.wait_recv()

        @pl.when((s >= 2 * split + 3) & odd)
        def _():
            for copy in extra(s, c, True):
                copy.wait()

        @pl.when(s == 2 * split + 3)
        def _():
            first_send.start()

        part = RB // 2
        pre = []
        for q in range(2):
            cc = jnp.dot(xv[pl.ds(r0 + q * part, part), :], uv[slot], preferred_element_type=F32)
            dh = lax.dot_general(zv[pl.ds(r0 + q * part, part), :], vv[slot], LAST, preferred_element_type=F32)
            pre.append((cc, dh))
        for q, (cc, dh) in enumerate(pre):
            h, slope = gelu_parts(cc.astype(BF16).astype(F32))
            h_st[sl, pl.ds(q * part, part), :] = h.astype(BF16)
            dc_st[sl, pl.ds(q * part, part), :] = (dh * slope).astype(BF16)

        @pl.when(ahead)
        def _():
            arrive_late(hc)

        @pl.when((half == 0) | (c < split))
        def _():
            acc[pl.ds(r0, RB), :] += lax.dot_general(dc_st[sl], uv[slot, near, :], LAST, preferred_element_type=F32)

        keep, push = outs(s, c, r0)
        for copy in keep + push:
            copy.start()

        @pl.when((half == 1) & (c == split))
        def _():
            for copy in extra(s, c, True):
                copy.start()

        @pl.when((half == 1) & (c > split))
        def _():
            for copy in extra(s, c, False):
                copy.start()

    for n in range(2):
        keep, push = outs(steps - 2 + n, 0, 0)
        for copy in keep:
            copy.wait()
        for copy in push:
            copy.wait_send()
            copy.wait_recv()
    for copy in extra(1, split, True):
        copy.wait()
    own_save.wait()
    part_send.wait_recv()
    part_send.wait_send()
    first_send.wait_recv()
    first_send.wait_send()
    drain(chunks - 4, chunks)


def hidden_call(x_act, w_up, w_down, z_grad):
    rows, dk = x_act.shape
    ffc = w_up.shape[1]
    ff, dq = w_down.shape
    chunks = ffc // W
    flops = 2 * rows * 2 * ff * dk * 5
    hbm = pl.BlockSpec(memory_space=pl.ANY)
    sds = jax.ShapeDtypeStruct
    out_shape = [
        sds((4 * rows, ff), BF16), sds((4 * rows, ffc), BF16), sds((4 * rows, dk), BF16), sds((4 * rows, dq), BF16),
        sds((rows, dk), F32), sds((rows, dk), F32), sds((rows, dk), F32),
        sds((rows, W), BF16), sds((rows, W), BF16), sds((rows, (PHI - 1) * W), BF16), sds((rows, PHI * W), BF16),
        sds((dk, W), BF16), sds((dk, (PHI - 1) * W), BF16), sds((dk, PHI * W), BF16),
        sds(w_up.shape, BF16), sds(w_up.shape, BF16), sds(w_up.shape, BF16),
        sds(w_down.shape, BF16), sds(w_down.shape, BF16), sds(w_down.shape, BF16),
    ]
    dma = pltpu.SemaphoreType.DMA
    return pl.pallas_call(
        hidden_kernel,
        in_specs=[hbm] * 4,
        out_specs=[hbm] * len(out_shape),
        out_shape=out_shape,
        scratch_shapes=[
            pltpu.VMEM((2 * rows, 2 * dk), BF16), pltpu.VMEM((2 * rows, 2 * dk), BF16),
            pltpu.VMEM((SLOTS, 2 * dk, 2 * W), BF16), pltpu.VMEM((SLOTS, 2 * W, 2 * dk), BF16),
            pltpu.VMEM((2 * rows, dk), F32),
            pltpu.VMEM((2, RB, 2 * W), BF16), pltpu.VMEM((2, RB, 2 * W), BF16),
            dma((6,)), dma((6,)), dma((chunks, 3)), dma((chunks, 3)), dma((chunks, 3)), dma((chunks, 3)),
            dma((10,)), dma((10,)), dma((12,)), dma((5,)), dma((2, 3)), dma((2,)), dma((2, 3)), dma((4 * ffc // (2 * W), 3)),
        ],
        compiler_params=pltpu.CompilerParams(
            collective_id=0, has_side_effects=True, vmem_limit_bytes=67_000_000),
        cost_estimate=pl.CostEstimate(flops=flops, bytes_accessed=200_000_000, transcendentals=2 * rows * ff),
        name="hidden",
    )(x_act, w_up, w_down, z_grad)


def solution(mesh):
    row_spec = P(("dp", "cx", "cz"), "cy")
    up_spec = P("cy", ("cz", "cx"))
    down_spec = P("cz", ("cy", "cx"))
    up_out = P(("dp", "cy"), ("cz", "cx"))
    down_out = P(("dp", "cz"), ("cy", "cx"))
    swap = [(0, 1), (1, 0)]

    def local_step(x_act, w_up, w_down, z_grad):
        (h, dc, xs, zs, dx_own, _, dx_got, _, dc_got, dcp_own, dcp_oth, up_y0, up_y, up_yd) = hidden_call(
            x_act, w_up, w_down, z_grad)[:14]
        dcr_own = lax.ppermute(dcp_own, "cz", swap)
        dcr_oth = lax.ppermute(dcp_oth, "cz", swap)
        down_grad = lax.dot_general(h, zs, FIRST, preferred_element_type=F32).astype(BF16)
        up_grad = lax.dot_general(xs, dc, FIRST, preferred_element_type=F32).astype(BF16)
        dx = lax.dot_general(dc_got, up_y0, LAST, preferred_element_type=F32) + (dx_own + dx_got)
        dx = lax.optimization_barrier(dx)
        dx = lax.dot_general(dcr_own, up_y, LAST, preferred_element_type=F32) + dx
        dx = lax.optimization_barrier(dx)
        x_grad = (lax.dot_general(dcr_oth, up_yd, LAST, preferred_element_type=F32) + dx).astype(BF16)
        return (x_grad, up_grad, down_grad)

    return jax.shard_map(local_step, mesh=mesh, in_specs=(row_spec, up_spec, down_spec, row_spec), out_specs=(row_spec, up_out, down_out), check_vma=False)
```

```python
import math
import jax
import jax.numpy as jnp
from jax import lax
from jax.experimental import pallas as pl
from jax.experimental.pallas import tpu as pltpu
from jax.sharding import PartitionSpec as P

GELU_COEF = 0.044715
SQRT_TWO_PI = math.sqrt(2.0 / math.pi)
LAST = (((1,), (1,)), ((), ()))
FIRST = (((0,), (0,)), ((), ()))
F32 = jnp.float32
BF16 = jnp.bfloat16
MESH = pl.DeviceIdType.MESH


W = 128
RB = 1024
PHI = 8
END = 3
AHEAD = 8
SLOTS = 8


def gelu_parts(c):
    c2 = c * c
    t = jnp.tanh(SQRT_TWO_PI * (c * (1.0 + GELU_COEF * c2)))
    half = 0.5 * (1.0 + t)
    slope = half + 0.5 * c * (1.0 - t * t) * SQRT_TWO_PI * (1.0 + 3.0 * GELU_COEF * c2)
    return c * half, slope


def hidden_kernel(x_in, up, down, z_in,
                  h_out, dc_out, x_out, z_out, dx_own, dx_part, dx_got, dc_first, dc_got, dcp_own, dcp_mid, dcp_end, up_y0, up_y, up_yd, up_ye, up_d, up_x, up_xd, down_d, down_x, down_xd,
                  xv, zv, uv, vv, acc, h_st, dc_st,
                  act_send, act_recv, wx_send, wx_recv, wd_send, wd_recv, all_send, all_recv,
                  load_sem, local_sem, out_sem, extra_sem, push_send, push_recv):
    cz, cy, cx = lax.axis_index("cz"), lax.axis_index("cy"), lax.axis_index("cx")
    to_x, to_y, to_d = {"cy": 1 - cy}, {"cz": 1 - cz}, {"cx": 1 - cx}
    rows, dk = x_in.shape
    ffc = up.shape[1]
    dq = down.shape[1]
    chunks = ffc // W

    def remote(src, dst, send, recv, dev):
        return pltpu.make_async_remote_copy(src_ref=src, dst_ref=dst, send_sem=send, recv_sem=recv,
                                            device_id=dev, device_id_type=MESH)

    def mine(c):
        return pl.ds(pl.multiple_of(c * W, W), W)

    def frow(f, c):
        return pl.ds(pl.multiple_of(f * ffc + c * W, W), W)

    own, oth = pl.ds(0, rows), pl.ds(rows, rows)
    near, far = pl.ds(0, dk), pl.ds(dk, dk)

    x1 = remote(x_in, xv.at[own, far], act_send.at[0], act_recv.at[0], to_x)
    z1 = remote(z_in, zv.at[own, far], act_send.at[1], act_recv.at[1], to_x)
    x2 = remote(x_in, xv.at[oth, near], act_send.at[2], act_recv.at[2], to_y)
    z2 = remote(z_in, zv.at[oth, near], act_send.at[3], act_recv.at[3], to_y)
    x3 = remote(xv.at[own, far], xv.at[oth, far], act_send.at[4], act_recv.at[4], to_y)
    z3 = remote(zv.at[own, far], zv.at[oth, far], act_send.at[5], act_recv.at[5], to_y)
    up_all = remote(up, up_d, all_send.at[0], all_recv.at[0], to_d)
    down_all = remote(down, down_d, all_send.at[1], all_recv.at[1], to_d)

    split = chunks - PHI
    mid = PHI - END
    head, tail = pl.ds(split * W, W), pl.ds((split + 1) * W, (PHI - 1) * W)
    up_tail = [remote(up.at[:, head], up_y0, all_send.at[2], all_recv.at[2], to_y),
               remote(up.at[:, tail], up_y, all_send.at[7], all_recv.at[7], to_y)]
    up_tail_d = [remote(up_y0, up_yd.at[:, pl.ds(0, W)], all_send.at[3], all_recv.at[3], to_d),
                 remote(up_y.at[:, pl.ds(0, (mid - 1) * W)], up_yd.at[:, pl.ds(W, (mid - 1) * W)],
                        all_send.at[8], all_recv.at[8], to_d),
                 remote(up_y.at[:, pl.ds((mid - 1) * W, END * W)], up_ye, all_send.at[10], all_recv.at[10], to_d)]
    first_send = remote(dc_first, dc_got, all_send.at[9], all_recv.at[9], to_y)
    part_save = pltpu.make_async_copy(acc.at[oth], dx_part, local_sem.at[3])
    part_send = remote(dx_part, dx_got, all_send.at[4], all_recv.at[4], to_y)
    own_save = pltpu.make_async_copy(acc.at[own], dx_own, local_sem.at[4])

    def over_x(c):
        return [remote(up.at[:, mine(c)], up_x.at[:, mine(c)], wx_send.at[c, 0], wx_recv.at[c, 0], to_x)] + [
            remote(down.at[frow(f, c)], down_x.at[frow(f, c)], wx_send.at[c, 1 + f], wx_recv.at[c, 1 + f], to_x)
            for f in range(2)]

    def over_d(c):
        return [remote(up_x.at[:, mine(c)], up_xd.at[:, mine(c)], wd_send.at[c, 0], wd_recv.at[c, 0], to_d)] + [
            remote(down_x.at[frow(f, c)], down_xd.at[frow(f, c)], wd_send.at[c, 1 + f], wd_recv.at[c, 1 + f], to_d)
            for f in range(2)]

    def lanes(part, core):
        return pl.ds(pl.multiple_of(part * dk + core * dq, 128), dq)

    def loads(c, late):
        slot = lax.rem(c, SLOTS)
        left, right = pl.ds(0, W), pl.ds(W, W)
        if late:
            moves = [(up_xd.at[:, mine(c)], uv.at[slot, far, right])]
            parts = [(down_xd, lanes(1, 1 - cx))]
        else:
            moves = [(up.at[:, mine(c)], uv.at[slot, near, left]),
                     (up_d.at[:, mine(c)], uv.at[slot, near, right]),
                     (up_x.at[:, mine(c)], uv.at[slot, far, left])]
            parts = [(down, lanes(0, cx)), (down_d, lanes(0, 1 - cx)), (down_x, lanes(1, cx))]
        for src, lane in parts:
            moves.append((src.at[frow(cx, c)], vv.at[slot, left, lane]))
            moves.append((src.at[frow(1 - cx, c)], vv.at[slot, right, lane]))
        base = 9 if late else 0
        return [pltpu.make_async_copy(s, d, load_sem.at[base + i]) for i, (s, d) in enumerate(moves)]

    barrier = pltpu.get_barrier_semaphore()
    for dev in (to_x, to_y, to_d):
        pl.semaphore_signal(barrier, inc=1, device_id=dev, device_id_type=MESH)
    pl.semaphore_wait(barrier, 3)

    x1.start()
    x2.start()
    z1.start()
    z2.start()
    for c in range(AHEAD):
        for copy in over_x(c):
            copy.start()
    up_all.start()
    down_all.start()
    x0 = pltpu.make_async_copy(x_in, xv.at[own, near], local_sem.at[0])
    z0 = pltpu.make_async_copy(z_in, zv.at[own, near], local_sem.at[1])
    x0.start()
    z0.start()

    @pl.loop(0, 2 * rows // 256)
    def _(i):
        acc[pl.ds(pl.multiple_of(i * 256, 256), 256), :] = jnp.zeros((256, dk), F32)

    x1.wait_recv()
    x3.start()
    z1.wait_recv()
    z3.start()
    for copy in up_tail:
        copy.start()
    x0.wait()
    z0.wait()
    up_all.wait_recv()
    down_all.wait_recv()
    mine_all, core_all = pl.ds(0, 2 * rows), pl.ds(2 * rows, 2 * rows)
    saves = [pltpu.make_async_copy(xv.at[:, near], x_out.at[mine_all], local_sem.at[0]),
             pltpu.make_async_copy(zv.at[:, lanes(0, cx)], z_out.at[mine_all], local_sem.at[1])]
    shares = [remote(xv.at[:, near], x_out.at[core_all], all_send.at[5], all_recv.at[5], to_d),
              remote(zv.at[:, lanes(0, 1 - cx)], z_out.at[core_all], all_send.at[6], all_recv.at[6], to_d)]

    def outs(n, c, r0):
        sl = lax.rem(n, 2)
        r = pl.ds(r0, RB)
        left, right = pl.ds(0, W), pl.ds(W, W)
        far_r = pl.ds(2 * rows + r0, RB)
        moves = ((h_st.at[sl, :, left], h_out.at[r, frow(cx, c)]), (h_st.at[sl, :, right], h_out.at[r, frow(1 - cx, c)]),
                 (dc_st.at[sl, :, left], dc_out.at[r, mine(c)]))
        pushes = ((h_st.at[sl, :, left], h_out.at[far_r, frow(cx, c)]), (h_st.at[sl, :, right], h_out.at[far_r, frow(1 - cx, c)]),
                  (dc_st.at[sl, :, right], dc_out.at[far_r, mine(c)]))
        return ([pltpu.make_async_copy(src, dst, out_sem.at[sl, i]) for i, (src, dst) in enumerate(moves)],
                [remote(src, dst, push_send.at[sl, i], push_recv.at[n, i], to_d) for i, (src, dst) in enumerate(pushes)])

    def extra(n, c, first, last):
        sl = lax.rem(n, 2)

        def block(start):
            return pl.ds(pl.multiple_of((c - start) * W, W), W)

        own_dst = dc_first if first else dcp_own.at[:, block(split + 1)]
        oth_dst = dcp_end.at[:, block(split + mid)] if last else dcp_mid.at[:, block(split)]
        return [pltpu.make_async_copy(dc_st.at[sl, :, pl.ds(0, W)], own_dst, extra_sem.at[0]),
                pltpu.make_async_copy(dc_st.at[sl, :, pl.ds(W, W)], oth_dst, extra_sem.at[1])]

    steps = 2 * chunks

    def drain(first, last):
        @pl.loop(first, last)
        def _(c):
            for copy in over_x(c) + over_d(c):
                copy.wait_send()

    @pl.loop(0, steps)
    def _(s):
        paired = s >= 2 * split
        c = jnp.where(paired, s // 2, jnp.where(s < SLOTS, s, jnp.where(s < SLOTS + split, s - SLOTS, s - split)))
        half = jnp.where(paired, lax.rem(s, 2), jnp.where((s >= SLOTS) & (s < SLOTS + split), 1, 0))
        odd = lax.rem(s, 2) == 1
        single = (s >= 2 * SLOTS - 1) & (s < SLOTS + split - 1)
        ahead = single | ((s >= 2 * split - 1) & odd & (s < steps - 1))
        hc = jnp.where(single, s - SLOTS + 1, (s + 1) // 2)

        def arrive(c):
            for copy in over_x(c):
                copy.wait_recv()
            for copy in over_d(c):
                copy.start()

            @pl.when(c + AHEAD < chunks)
            def _():
                for copy in over_x(c + AHEAD):
                    copy.start()

            for copy in loads(c, False):
                copy.start()

        def arrive_late(c):
            for copy in over_d(c):
                copy.wait_recv()
            for copy in loads(c, True):
                copy.start()

        @pl.when(s < SLOTS)
        def _():
            arrive(s)
            arrive_late(s)

        @pl.when((s < SLOTS) | ((s >= 2 * SLOTS) & (s < SLOTS + split)) | (paired & ~odd))
        def _():
            for copy in loads(c, False) + loads(c, True):
                copy.wait()

        @pl.when(s == SLOTS + split)
        def _():
            part_save.start()
            for copy in up_tail:
                copy.wait_recv()
            for copy in up_tail_d:
                copy.start()
            part_save.wait()
            part_send.start()

        @pl.when(ahead)
        def _():
            arrive(hc)

        @pl.when(s == SLOTS)
        def _():
            x2.wait_recv()
            z2.wait_recv()
            for copy in saves + shares:
                copy.start()
            x3.wait_recv()
            z3.wait_recv()

        @pl.when(s == steps - 4)
        def _():
            for copy in saves:
                copy.wait()
            for copy in shares:
                copy.wait_send()
                copy.wait_recv()
            for copy in up_tail_d:
                copy.wait_recv()
            for copy in [x1, z1, x2, z2, x3, z3, up_all, down_all] + up_tail + up_tail_d:
                copy.wait_send()
            drain(0, chunks - 4)

        @pl.when(s == steps - 1)
        def _():
            own_save.start()

        slot = lax.rem(c, SLOTS)
        r0 = pl.multiple_of(half * rows, RB)
        sl = lax.rem(s, 2)

        @pl.when(s >= 2)
        def _():
            keep, push = outs(s - 2, c, r0)
            for copy in keep:
                copy.wait()
            for copy in push:
                copy.wait_send()
                copy.wait_recv()

        @pl.when((s >= 2 * split + 3) & odd)
        def _():
            for copy in extra(s, split, True, False):
                copy.wait()

        @pl.when(s == 2 * split + 3)
        def _():
            first_send.start()

        part = RB // 2
        pre = []
        for q in range(2):
            cc = jnp.dot(xv[pl.ds(r0 + q * part, part), :], uv[slot], preferred_element_type=F32)
            dh = lax.dot_general(zv[pl.ds(r0 + q * part, part), :], vv[slot], LAST, preferred_element_type=F32)
            pre.append((cc, dh))
        for q, (cc, dh) in enumerate(pre):
            h, slope = gelu_parts(cc.astype(BF16).astype(F32))
            h_st[sl, pl.ds(q * part, part), :] = h.astype(BF16)
            dc_st[sl, pl.ds(q * part, part), :] = (dh * slope).astype(BF16)

        @pl.when(ahead)
        def _():
            arrive_late(hc)

        @pl.when((half == 0) | (c < split))
        def _():
            acc[pl.ds(r0, RB), :] += lax.dot_general(dc_st[sl], uv[slot, near, :], LAST, preferred_element_type=F32)

        keep, push = outs(s, c, r0)
        for copy in keep + push:
            copy.start()

        @pl.when((half == 1) & (c == split))
        def _():
            for copy in extra(s, c, True, False):
                copy.start()

        @pl.when((half == 1) & (c > split) & (c < split + mid))
        def _():
            for copy in extra(s, c, False, False):
                copy.start()

        @pl.when((half == 1) & (c >= split + mid))
        def _():
            for copy in extra(s, c, False, True):
                copy.start()

    for n in range(2):
        keep, push = outs(steps - 2 + n, 0, 0)
        for copy in keep:
            copy.wait()
        for copy in push:
            copy.wait_send()
            copy.wait_recv()
    for copy in extra(1, split, True, False):
        copy.wait()
    own_save.wait()
    part_send.wait_recv()
    part_send.wait_send()
    first_send.wait_recv()
    first_send.wait_send()
    drain(chunks - 4, chunks)


def hidden_call(x_act, w_up, w_down, z_grad):
    rows, dk = x_act.shape
    ffc = w_up.shape[1]
    ff, dq = w_down.shape
    chunks = ffc // W
    flops = 2 * rows * 2 * ff * dk * 5
    hbm = pl.BlockSpec(memory_space=pl.ANY)
    sds = jax.ShapeDtypeStruct
    out_shape = [
        sds((4 * rows, ff), BF16), sds((4 * rows, ffc), BF16), sds((4 * rows, dk), BF16), sds((4 * rows, dq), BF16),
        sds((rows, dk), F32), sds((rows, dk), F32), sds((rows, dk), F32),
        sds((rows, W), BF16), sds((rows, W), BF16), sds((rows, (PHI - 1) * W), BF16),
        sds((rows, (PHI - END) * W), BF16), sds((rows, END * W), BF16),
        sds((dk, W), BF16), sds((dk, (PHI - 1) * W), BF16),
        sds((dk, (PHI - END) * W), BF16), sds((dk, END * W), BF16),
        sds(w_up.shape, BF16), sds(w_up.shape, BF16), sds(w_up.shape, BF16),
        sds(w_down.shape, BF16), sds(w_down.shape, BF16), sds(w_down.shape, BF16),
    ]
    dma = pltpu.SemaphoreType.DMA
    return pl.pallas_call(
        hidden_kernel,
        in_specs=[hbm] * 4,
        out_specs=[hbm] * len(out_shape),
        out_shape=out_shape,
        scratch_shapes=[
            pltpu.VMEM((2 * rows, 2 * dk), BF16), pltpu.VMEM((2 * rows, 2 * dk), BF16),
            pltpu.VMEM((SLOTS, 2 * dk, 2 * W), BF16), pltpu.VMEM((SLOTS, 2 * W, 2 * dk), BF16),
            pltpu.VMEM((2 * rows, dk), F32),
            pltpu.VMEM((2, RB, 2 * W), BF16), pltpu.VMEM((2, RB, 2 * W), BF16),
            dma((6,)), dma((6,)), dma((chunks, 3)), dma((chunks, 3)), dma((chunks, 3)), dma((chunks, 3)),
            dma((11,)), dma((11,)), dma((12,)), dma((5,)), dma((2, 3)), dma((2,)), dma((2, 3)), dma((4 * ffc // (2 * W), 3)),
        ],
        compiler_params=pltpu.CompilerParams(
            collective_id=0, has_side_effects=True, vmem_limit_bytes=67_000_000),
        cost_estimate=pl.CostEstimate(flops=flops, bytes_accessed=200_000_000, transcendentals=2 * rows * ff),
        name="hidden",
    )(x_act, w_up, w_down, z_grad)


def solution(mesh):
    row_spec = P(("dp", "cx", "cz"), "cy")
    up_spec = P("cy", ("cz", "cx"))
    down_spec = P("cz", ("cy", "cx"))
    up_out = P(("dp", "cy"), ("cz", "cx"))
    down_out = P(("dp", "cz"), ("cy", "cx"))
    swap = [(0, 1), (1, 0)]

    def local_step(x_act, w_up, w_down, z_grad):
        (h, dc, xs, zs, dx_own, _, dx_got, _, dc_got, dcp_own, dcp_mid, dcp_end, up_y0, up_y, up_yd, up_ye) = hidden_call(
            x_act, w_up, w_down, z_grad)[:16]
        dcr_own = lax.ppermute(dcp_own, "cz", swap)
        dcr_mid = lax.ppermute(dcp_mid, "cz", swap)
        dcr_end = lax.ppermute(dcp_end, "cz", swap)
        down_grad = lax.dot_general(h, zs, FIRST, preferred_element_type=F32).astype(BF16)
        up_grad = lax.dot_general(xs, dc, FIRST, preferred_element_type=F32).astype(BF16)
        dx = lax.dot_general(dc_got, up_y0, LAST, preferred_element_type=F32) + (dx_own + dx_got)
        dx = lax.optimization_barrier(dx)
        dx = lax.dot_general(dcr_own, up_y, LAST, preferred_element_type=F32) + dx
        dx = lax.optimization_barrier(dx)
        dx = lax.dot_general(dcr_mid, up_yd, LAST, preferred_element_type=F32) + dx
        dx = lax.optimization_barrier(dx)
        x_grad = (lax.dot_general(dcr_end, up_ye, LAST, preferred_element_type=F32) + dx).astype(BF16)
        return (x_grad, up_grad, down_grad)

    return jax.shard_map(local_step, mesh=mesh, in_specs=(row_spec, up_spec, down_spec, row_spec), out_specs=(row_spec, up_out, down_out), check_vma=False)
```
